512 devices in a mesh: rad: 16 (over z_hi, x, core), harm: 32 (over y, z_lo).
Axes of the slice: x: 4, y: 8, z: 8 (z_hi: 2, z_lo: 4; z = z_hi * 4 + z_lo), core: 2. Of those that a mesh axis runs over, the one named last changes fastest.
Arguments:
- velocity: bfloat16 [3, 64, 2, 256, 256], P(None, 'rad', None, 'harm'), may hold values from -6 to 6
- magnetic: bfloat16 [3, 64, 2, 256, 256], P(None, 'rad', None, 'harm'), may hold values from -6 to 6
- vorticity: bfloat16 [3, 64, 2, 256, 256], P(None, 'rad', None, 'harm'), may hold values from -6 to 6
- current: bfloat16 [3, 64, 2, 256, 256], P(None, 'rad', None, 'harm'), may hold values from -6 to 6
Outputs:
- advection: bfloat16 [3, 64, 2, 256, 256], P(None, 'rad', None, 'harm')
- induction_gradient: bfloat16 [3, 64, 2, 256, 256], P(None, 'rad', None, 'harm')
- energy_spectra: float32 [2, 64, 256], P(None, 'rad')
The draws below stay inside these ranges and needn't reach their ends.
All inputs are finite; a program needn't handle non-finite values.
Results may differ from the reference program's by a relative error of at most 0.01.
Values may be sent and summed in bfloat16 or wider, within the bound.
A program may use at most 64 MiB of HBM per device.

```python
import jax
import jax.numpy as jnp
from jax import lax

L = 256
NTHETA = 384
NPHI = 768
NR = 64


def block_scale(stream_key, extent, split, low, largest):
    factor_of = 1.0
    for axis_at, parts in split:
        draws = jax.random.uniform(jax.random.fold_in(jax.random.fold_in(stream_key, 6), axis_at), (parts,), jnp.float32, low / len(split), largest / len(split))
        factor_of = factor_of * jnp.repeat(jnp.exp(draws), extent[axis_at] // parts).reshape((-1,) + (1,) * (len(extent) - 1 - axis_at))
    return factor_of


def scatter_about(own_key, dims, scale, most, shards=(), held_as=jnp.bfloat16):
    level = block_scale(own_key, dims, shards, -0.22, 0.18) if shards else 1.0
    values = jax.random.normal(own_key, dims, jnp.float32) * scale * level
    return jnp.minimum(jnp.maximum(values, -most), most).astype(held_as)


def setup_inputs(seed: int = 0) -> dict:
    splits = jax.random.split(jax.random.key(seed), 5)
    return {
        "velocity": scatter_about(splits[0], (3, NR, 2, L, L), 1.0, 6.0, ((1, 16), (3, 32))),
        "magnetic": scatter_about(splits[1], (3, NR, 2, L, L), 1.0, 6.0, ((1, 16), (3, 32))),
        "vorticity": scatter_about(splits[2], (3, NR, 2, L, L), 1.0, 6.0, ((1, 16), (3, 32))),
        "current": scatter_about(splits[3], (3, NR, 2, L, L), 1.0, 6.0, ((1, 16), (3, 32))),
    }


def north_table(order_ints, degree_count, theta_count):
    half_rows = theta_count // 2
    row_index = jnp.arange(half_rows, dtype=jnp.float32)
    angles = jnp.pi * (row_index + 0.5) / theta_count
    cosine = jnp.cos(angles)
    sine_theta = jnp.sin(angles)
    order_float = order_ints.astype(jnp.float32)[:, None]
    steps_k = jnp.arange(1, degree_count, dtype=jnp.int32)
    steps_float = steps_k.astype(jnp.float32)
    log_terms = 0.5 * jnp.log((2.0 * steps_float + 1.0) / (2.0 * steps_float))
    log_taken = jnp.where(steps_k[None, :] <= order_ints[:, None], log_terms[None, :], 0.0)
    log_start = 0.5 * jnp.log(jnp.float32(0.5)) + lax.optimization_barrier(jnp.sum(log_taken, axis=1))
    log_sector = log_start[:, None] + order_float * jnp.log(sine_theta)[None, :]
    sectoral = jnp.exp(jnp.maximum(log_sector, -60.0))
    unscale = jnp.exp(jnp.minimum(log_sector + 60.0, 0.0))
    order_col = order_ints[:, None]
    blocks = 16
    per_block = degree_count // blocks

    def advance(state_pair, block_index):
        latest, before = state_pair
        produced = []
        for inner_step in range(per_block):
            degree = block_index * per_block + inner_step
            degree_float = degree.astype(jnp.float32)
            general = degree > order_col + 1
            degree_square = degree_float * degree_float
            order_square = order_float * order_float
            ratio_upper = jnp.where(general, (4.0 * degree_square - 1.0) / jnp.where(general, degree_square - order_square, 1.0), 1.0)
            lower_degree = degree_float - 1.0
            ratio_lower = jnp.where(general, (lower_degree * lower_degree - order_square) / (4.0 * lower_degree * lower_degree - 1.0), 0.0)
            value_general = jnp.sqrt(ratio_upper) * (cosine[None, :] * latest - jnp.sqrt(ratio_lower) * before)
            first_up = jnp.sqrt(2.0 * order_float + 3.0) * cosine[None, :] * sectoral
            new_value = jnp.where(degree < order_col, 0.0, jnp.where(degree == order_col, sectoral, jnp.where(degree == order_col + 1, first_up, value_general)))
            before = latest
            latest = new_value
            produced.append(new_value)
        return ((latest, before), jnp.stack(produced))
    zero_rows = jnp.zeros((order_ints.shape[0], half_rows), jnp.float32)
    state_pair, legendre_raw = lax.scan(advance, (zero_rows, zero_rows), jnp.arange(blocks, dtype=jnp.int32))
    legendre_raw = legendre_raw.reshape(degree_count, order_ints.shape[0], half_rows)
    return jnp.transpose(legendre_raw, (1, 0, 2)) * unscale[:, None, :]

def full_table(north_rows, order_ints):
    degree_count = north_rows.shape[1]
    degrees = jnp.arange(degree_count, dtype=jnp.int32)
    parity = (degrees[None, :] + order_ints[:, None]) % 2
    sign_factor = (1 - 2 * parity).astype(jnp.float32)[:, :, None]
    return jnp.concatenate([north_rows, sign_factor * jnp.flip(north_rows, 2)], 2)

def quadrature(theta_count):
    half_rows = theta_count // 2
    row_index = jnp.arange(half_rows, dtype=jnp.float32)
    angles = jnp.pi * (row_index + 0.5) / theta_count
    wave_number = jnp.arange(1, half_rows + 1, dtype=jnp.float32)
    series = jnp.cos(2.0 * wave_number[None, :] * angles[:, None]) / (4.0 * wave_number[None, :] * wave_number[None, :] - 1.0)
    north_weights = 2.0 / theta_count * (1.0 - 2.0 * lax.optimization_barrier(jnp.sum(series, axis=1)))
    return jnp.concatenate([north_weights, jnp.flip(north_weights, 0)], 0)

def trig_table(degree_count, phi_count):
    orders = jnp.arange(degree_count, dtype=jnp.int32)[:, None]
    points = jnp.arange(phi_count, dtype=jnp.int32)[None, :]
    phase_angle = 2.0 * jnp.pi * (orders * points % phi_count).astype(jnp.float32) / phi_count
    return jnp.stack([jnp.cos(phase_angle), jnp.sin(phase_angle)]).astype(jnp.bfloat16)

def analysis_factor(order_ints, row_weights, degree_count, phi_count):
    mode_weight = jnp.where(order_ints == 0, 1.0, 2.0).astype(jnp.float32)
    return mode_weight[:, None] * float(degree_count) * row_weights[None, :] / float(phi_count)

def energy_weights(order_ints, degree_count):
    degrees = jnp.arange(degree_count, dtype=jnp.int32)
    order_col = order_ints[:, None]
    live_part = (degrees[None, :] >= order_col).astype(jnp.float32)
    inverse_modes = 1.0 / (2.0 * degrees.astype(jnp.float32) + 1.0)
    cosine_weight = jnp.where(order_col == 0, 0.5, 1.0)
    sine_weight = jnp.where(order_col == 0, 0.0, 1.0)
    return jnp.stack([cosine_weight * live_part * inverse_modes[None, :], sine_weight * live_part * inverse_modes[None, :]]).astype(jnp.float32)

def cross_product(first_vec, second_vec):
    return [first_vec[1] * second_vec[2] - first_vec[2] * second_vec[1], first_vec[2] * second_vec[0] - first_vec[0] * second_vec[2], first_vec[0] * second_vec[1] - first_vec[1] * second_vec[0]]

def nonlinear_terms(components):
    velocity_vec = components[0:3]
    magnetic_vec = components[3:6]
    vorticity_vec = components[6:9]
    current_vec = components[9:12]
    lamb_term = cross_product(velocity_vec, vorticity_vec)
    lorentz_term = cross_product(current_vec, magnetic_vec)
    induced = cross_product(velocity_vec, magnetic_vec)
    return [lamb_term[index_c] + lorentz_term[index_c] for index_c in range(3)] + induced

def rounded(values):
    return lax.optimization_barrier(values.astype(jnp.bfloat16)).astype(jnp.float32)

def reference(velocity, magnetic, vorticity, current):
    all_orders = jnp.arange(L, dtype=jnp.int32)
    north_rows = north_table(all_orders, L, NTHETA)
    legendre = rounded(full_table(north_rows, all_orders))
    trig_rows = lax.optimization_barrier(trig_table(L, NPHI)).astype(jnp.float32)
    factor = analysis_factor(all_orders, quadrature(NTHETA), L, NPHI)
    energy_weight = energy_weights(all_orders, L)
    fields = jnp.concatenate([velocity, magnetic, vorticity, current], 0)
    per_shell = jnp.moveaxis(fields, 1, 0)

    def one_shell(spectrum):
        mode_rows = jnp.einsum('crml,mlt->crmt', spectrum.astype(jnp.float32), legendre) * (1.0 / L)
        mode_rows = rounded(mode_rows)
        grid_values = jnp.einsum('crmt,rmp->ctp', mode_rows, trig_rows)
        products = rounded(jnp.stack(nonlinear_terms([grid_values[index_c] for index_c in range(12)])))
        analysed = jnp.einsum('ctp,rmp->crmt', products, trig_rows) * factor[None, None]
        analysed = rounded(analysed)
        spectra = jnp.einsum('crmt,mlt->crml', analysed, legendre)
        square = spectrum[:6].astype(jnp.float32) ** 2
        kinetic = lax.optimization_barrier(jnp.sum(square[:3] * energy_weight[None], axis=(0, 1, 2)))
        magnetic_energy = lax.optimization_barrier(jnp.sum(square[3:] * energy_weight[None], axis=(0, 1, 2)))
        return (spectra[:3].astype(jnp.bfloat16), spectra[3:].astype(jnp.bfloat16), jnp.stack([kinetic, magnetic_energy]))
    advection, induction, energy = lax.map(one_shell, per_shell)
    induction_wide = induction.astype(jnp.float32)
    padded = jnp.pad(induction_wide, ((1, 1), (0, 0), (0, 0), (0, 0), (0, 0)))
    gradient = ((padded[2:] - padded[:-2]) * 0.5).astype(jnp.bfloat16)
    return (jnp.moveaxis(advection, 0, 1), jnp.moveaxis(gradient, 0, 1), jnp.moveaxis(energy, 0, 1))
```

```python
import functools

import jax
import jax.numpy as jnp
from jax import lax
from jax.experimental import pallas as pl
from jax.experimental.pallas import tpu as pltpu
from jax.sharding import PartitionSpec as P

F32 = jnp.float32
BF16 = jnp.bfloat16
PI = 3.14159265358979
L = 256
HARM = 32
RAD = 16
NPHI = 768
CROW = 64


def sin_poly(y):
    z = y * y
    s = -1.0 / 39916800.0
    for c in (1.0 / 362880.0, -1.0 / 5040.0, 1.0 / 120.0, -1.0 / 6.0, 1.0):
        s = s * z + c
    return y * s


def cos_768(q):
    return sin_poly((192.0 - jnp.minimum(q, 768.0 - q)) * (PI / 384.0))


def mod_768(v):
    return v - 768.0 * jnp.floor((v + 0.5) * (1.0 / 768.0))


def iota(shape, dim):
    return lax.broadcasted_iota(jnp.int32, shape, dim)


def fiota(shape, dim):
    return iota(shape, dim).astype(F32)


def parity_sign(order):
    return 1.0 - 2.0 * ((iota((1, L), 1) + order) & 1).astype(F32)


def legendre_steps(me, tab):
    order = (me * 8 + iota((8, 128), 0)).astype(F32)
    order_sq = order * order
    degree = fiota((8, L), 1)
    own = (me * 8 + iota((8, L), 0)).astype(F32)
    logs = 0.5 * jnp.log((2.0 * degree + 1.0) / jnp.maximum(2.0 * degree, 1.0))
    taken = jnp.where((degree >= 1.0) & (degree <= own), logs, 0.0)
    log_start = 0.5 * jnp.log(jnp.full((8, 1), 0.5, F32)) + jnp.sum(taken, axis=1, keepdims=True)
    cosine, sector, unscale = [], [], []
    for jt in range(2):
        odd = 2.0 * (fiota((8, 128), 1) + 128.0 * jt) + 1.0
        cosine.append(sin_poly((384.0 - odd) * (PI / 768.0)))
        sine = sin_poly(jnp.minimum(odd, 768.0 - odd) * (PI / 768.0))
        log_sector = log_start + order * jnp.log(sine)
        sector.append(jnp.exp(jnp.maximum(log_sector, -60.0)))
        unscale.append(jnp.exp(jnp.minimum(log_sector + 60.0, 0.0)))
    zero = jnp.zeros((8, 128), F32)
    per = 16

    def block(index, state):
        q0, p0, q1, p1, back = state
        for inner in range(per):
            deg_i = index * per + inner
            deg = deg_i.astype(F32)
            sq = deg * deg
            live = order < deg
            t = (4.0 * sq - 1.0) / jnp.where(live, sq - order_sq, 1.0)
            a = jnp.where(live, jnp.sqrt(t), 0.0)
            ab = a * back
            back = jnp.where(live, lax.rsqrt(t), 0.0)
            start = order == deg
            n0 = a * cosine[0] * q0 + (jnp.where(start, sector[0], 0.0) - ab * p0)
            n1 = a * cosine[1] * q1 + (jnp.where(start, sector[1], 0.0) - ab * p1)
            row = pl.ds(pl.multiple_of(deg_i * 8, 8), 8)
            tab[0, row, :] = n0 * unscale[0]
            tab[1, row, :] = n1 * unscale[1]
            q0, p0, q1, p1 = n0, q0, n1, q1
        return q0, p0, q1, p1, back

    lax.fori_loop(0, L // per, block, (zero, zero, zero, zero, zero))


def kernel(
    vel, mag, vor, cur,
    adv, grad, energy,
    tab, qt, coef, rhs, synth, wire, modes, trig, turned, grid, prod, spec, back, backf,
    zed, out, ind, low, high, esrc, erecv, ered, efin,
    mode_send, mode_recv, spec_send, spec_recv, halo_send, halo_recv, e_send, e_recv,
):
    me = lax.axis_index("harm")
    my_rad = lax.axis_index("rad")
    up = lax.rem(my_rad + 1, RAD)
    down = lax.rem(my_rad + RAD - 1, RAD)

    def peer(i):
        return lax.rem(me + i, HARM)

    barrier = pltpu.get_barrier_semaphore()

    def greet(i, carry):
        pl.semaphore_signal(barrier, inc=1, device_id={"harm": peer(i)})
        return carry

    lax.fori_loop(1, HARM, greet, 0)
    pl.semaphore_signal(barrier, inc=1, device_id={"rad": up})
    pl.semaphore_signal(barrier, inc=1, device_id={"rad": down})

    coef[:, 0:CROW, :] = jnp.zeros((2, CROW, 128), F32)
    coef[:, CROW + 768:, :] = jnp.zeros((2, CROW, 128), F32)
    for a, ref in enumerate((vel, mag, vor, cur)):
        for half in range(2):
            lanes = pl.ds(half * 128, 128)
            coef[half, CROW + 192 * a:CROW + 192 * (a + 1), :] = (
                ref[:, :, :, :, lanes].astype(F32).reshape(192, 128)
            )

    legendre_steps(me, tab)

    row8 = iota((8, 128), 0)

    def synthesis(m, carry):
        for jt, rows in ((0, 128), (1, 64)):
            table = tab[jt, pl.ds(m, L, stride=8), :]
            qt[m, jt * 128:jt * 128 + rows, :] = table.T[0:rows].astype(BF16)
        sign = parity_sign(m)
        for r in range(2):
            for half in range(2):
                sgn = sign[:, half * 128:(half + 1) * 128]
                before = None
                for c in range(-1, 12):
                    rows = coef[half, pl.ds(CROW + c * 64 + r * 8 + m, 8, stride=16), :]
                    if c >= 0:
                        base = r * 192 + c * 16
                        for gn, part in ((0, jnp.where(row8 < 4, rows, 0.0)),
                                         (1, jnp.where(row8 >= 4, before, 0.0))):
                            lane = gn * 256 + half * 128
                            rhs[base:base + 16, lane:lane + 128] = jnp.concatenate(
                                [part, part * sgn], axis=0
                            ).astype(BF16)
                    before = rows
        lhs = jnp.concatenate([qt[m, 0:96, :], qt[m, 96:192, :]], axis=1)
        made = lax.dot_general(
            lhs, rhs[...], (((1,), (1,)), ((), ())), preferred_element_type=F32
        ) * (1.0 / L)
        for k in range(3):
            for lt in range(3):
                synth[k, lt, pl.ds(m, 32, stride=8), :] = made[
                    k * 32:(k + 1) * 32, lt * 128:(lt + 1) * 128
                ]
        return carry

    lax.fori_loop(0, 8, synthesis, 0)
    wire[...] = synth[...].astype(BF16)

    pl.semaphore_wait(barrier, HARM + 1)

    def rows_of(device):
        return pl.ds(pl.multiple_of(device * 8, 8), 8)

    def mode_copy(k, i):
        to = peer(i)
        return pltpu.make_async_remote_copy(
            src_ref=wire.at[k, :, rows_of(to), :],
            dst_ref=modes.at[k, :, rows_of(me), :],
            send_sem=mode_send.at[k],
            recv_sem=mode_recv.at[k],
            device_id={"harm": to},
        )

    for k in range(3):
        def send_modes(i, carry, k=k):
            mode_copy(k, i).start()
            return carry

        lax.fori_loop(1, HARM, send_modes, 0)
        pltpu.make_async_copy(
            wire.at[k, :, rows_of(me), :], modes.at[k, :, rows_of(me), :], mode_recv.at[k]
        ).start()

    order8 = me * 8 + iota((8, 128), 0)
    for half in range(2):
        degree = iota((8, 128), 1) + 128 * half
        weight = jnp.where(degree >= order8, 1.0 / (2.0 * degree.astype(F32) + 1.0), 0.0)
        weights = (
            weight * jnp.where(order8 == 0, 0.5, 1.0),
            weight * jnp.where(order8 == 0, 0.0, 1.0),
        )
        for q in range(2):
            for s in range(4):
                total = jnp.zeros((8, 128), F32)
                for c in range(3):
                    for r in range(2):
                        at = CROW + (((q * 3 + c) * 4 + s) * 2 + r) * 8
                        value = coef[half, at:at + 8, :]
                        total += value * value * weights[r]
                esrc[(q * 4 + s) * 2 + half] = jnp.sum(total, axis=0, keepdims=True)

    def energy_copy(i):
        to = peer(i)
        return pltpu.make_async_remote_copy(
            src_ref=esrc.at[lax.rem(to, 16)],
            dst_ref=erecv.at[me],
            send_sem=e_send.at[0],
            recv_sem=e_recv.at[0],
            device_id={"harm": to},
        )

    def send_energy(i, carry):
        energy_copy(i).start()
        return carry

    lax.fori_loop(1, HARM, send_energy, 0)
    pltpu.make_async_copy(esrc.at[lax.rem(me, 16)], erecv.at[me], e_recv.at[0]).start()

    def trig_rows(b, carry):
        angle = mod_768((b * 8 + iota((8, NPHI), 0)).astype(F32) * fiota((8, NPHI), 1))
        rows = pl.ds(pl.multiple_of(b * 8, 8), 8)
        trig[0, rows, :] = cos_768(angle).astype(BF16)
        trig[1, rows, :] = cos_768(jnp.where(angle >= 192.0, angle - 192.0, angle + 576.0)).astype(BF16)
        return carry

    lax.fori_loop(0, 32, trig_rows, 0)

    lane = iota((1, 128), 1)
    factors = []
    for k in range(3):
        row = ((lane >> 2) & 1) * 96 + k * 32 + me
        wave = fiota((192, 128), 0) + 1.0
        odd = (2 * row + 1).astype(F32)
        series = cos_768(mod_768(wave * odd)) / (4.0 * wave * wave - 1.0)
        weight = (2.0 / 384.0) * (1.0 - 2.0 * jnp.sum(series, axis=0, keepdims=True))
        factors.append(weight * (256.0 / 768.0))

    def grid_of(k):
        for lt in range(3):
            turned[lt * 128:(lt + 1) * 128, :] = modes[k, lt].T
        grid[...] = jnp.dot(turned[0:192], trig[0], preferred_element_type=F32) + jnp.dot(
            turned[192:384], trig[1], preferred_element_type=F32
        )
        for pt in range(6):
            cols = slice(pt * 128, (pt + 1) * 128)
            g = [grid[c * 16:(c + 1) * 16, cols] for c in range(12)]
            u, b, w, j = g[0:3], g[3:6], g[6:9], g[9:12]

            def cross(x, y, i):
                n, o = (i + 1) % 3, (i + 2) % 3
                return x[n] * y[o] - x[o] * y[n]

            for c in range(6):
                value = cross(u, w, c) + cross(j, b, c) if c < 3 else cross(u, b, c - 3)
                value = value.astype(BF16)
                ends = (96, ) if c < 2 else (128 - 32, 192 - 32)
                prod[c * 16:(c + 1) * 16, cols] = value
                for end in ends:
                    prod[end + c * 16:end + (c + 1) * 16, cols] = value

    even = iota((256, 1), 0)
    mode_weight = jnp.where(even == 0, 1.0, 2.0)
    wide_lane = iota((1, 128), 1)

    def analysed(k):
        cosine = lax.dot_general(
            trig[0], prod[0:128], (((1,), (1,)), ((), ())), preferred_element_type=F32
        )
        sine = lax.dot_general(
            trig[1], prod[...], (((1,), (1,)), ((), ())), preferred_element_type=F32
        )
        scale = mode_weight * factors[k]
        first = jnp.where(wide_lane < 96, cosine, sine[:, 0:128]) * scale
        second = sine[:, 128:256] * scale
        return first.astype(BF16), second

    def wait_modes(k):
        pltpu.make_async_copy(modes.at[k], modes.at[k], mode_recv.at[k]).wait()

    def spec_copy(part, tiles, i):
        to = peer(i)
        return pltpu.make_async_remote_copy(
            src_ref=spec.at[tiles, rows_of(to), :],
            dst_ref=back.at[tiles, rows_of(me), :],
            send_sem=spec_send.at[part],
            recv_sem=spec_recv.at[part],
            device_id={"harm": to},
        )

    def send_spectra(part, tiles):
        def one(i, carry):
            spec_copy(part, tiles, i).start()
            return carry

        lax.fori_loop(1, HARM, one, 0)
        pltpu.make_async_copy(
            spec.at[tiles, rows_of(me), :], back.at[tiles, rows_of(me), :], spec_recv.at[part]
        ).start()

    tiles_a, tiles_b = pl.ds(0, 3), pl.ds(3, 2)
    wait_modes(0)
    grid_of(0)
    first, second0 = analysed(0)
    spec[0] = first
    spec[1] = second0.astype(BF16)
    wait_modes(1)
    grid_of(1)
    first, second1 = analysed(1)
    spec[2] = first
    spec[1] = jnp.where(wide_lane < 64, spec[1].astype(F32), second1).astype(BF16)
    send_spectra(0, tiles_a)

    pltpu.make_async_copy(erecv, erecv, e_recv.at[0]).wait()
    ered[...] = jnp.sum(erecv[...], axis=0, keepdims=True)
    mine = lax.rem(me, 16)

    def row_copy(i):
        to = me - mine + lax.rem(mine + i, 16)
        return pltpu.make_async_remote_copy(
            src_ref=ered.at[0],
            dst_ref=efin.at[mine],
            send_sem=e_send.at[1],
            recv_sem=e_recv.at[1],
            device_id={"harm": to},
        )

    def send_row(i, carry):
        row_copy(i).start()
        return carry

    lax.fori_loop(1, 16, send_row, 0)
    pltpu.make_async_copy(ered.at[0], efin.at[mine], e_recv.at[1]).start()

    wait_modes(2)
    grid_of(2)
    first, second2 = analysed(2)
    spec[3] = first
    spec[4] = second2.astype(BF16)
    send_spectra(1, tiles_b)

    def wait_spectra(part, tiles):
        pltpu.make_async_copy(back.at[tiles], back.at[tiles], spec_recv.at[part]).wait()

    wait_spectra(0, tiles_a)
    backf[0:3] = back[0:3].astype(F32)
    wait_spectra(1, tiles_b)
    backf[3:5] = back[3:5].astype(F32)

    lane_row = iota((32, 128), 1)
    gn_of = (lane_row >> 2) & 1

    def latitude(m, carry):
        tiles = [backf[t, pl.ds(m, 32, stride=8), :] for t in range(5)]
        middle = (
            jnp.where(lane_row < 64, tiles[1], 0.0),
            jnp.where(lane_row >= 64, tiles[1], 0.0),
            jnp.where(lane_row < 64, tiles[4], 0.0),
        )
        lead = (tiles[0], tiles[2], tiles[3])
        for gn in range(2):
            for k in range(3):
                at = (gn * 3 + k) * 32
                zed[at:at + 32, 0:128] = jnp.where(gn_of == gn, lead[k], 0.0).astype(BF16)
                zed[at:at + 32, 128:256] = jnp.where(gn_of == gn, middle[k], 0.0).astype(BF16)
        sums = lax.dot_general(
            zed[...], qt[m], (((0,), (0,)), ((), ())), preferred_element_type=F32
        )
        sums = jnp.concatenate([sums[0:128], sums[128:192] + sums[192:256]], axis=0)
        sign = parity_sign(m)
        for r in range(2):
            for c in range(6):
                base = r * 96 + c * 16
                both = sums[base:base + 8] + sums[base + 8:base + 16] * sign
                both = both[0:4] + both[4:8]
                for half in range(2):
                    out[half, pl.ds(c * 64 + r * 8 + m, 4, stride=16), :] = both[
                        :, half * 128:(half + 1) * 128
                    ]
        return carry

    lax.fori_loop(0, 8, latitude, 0)

    for half in range(2):
        lanes = pl.ds(half * 128, 128)
        ind[:, :, :, :, lanes] = out[half, 192:384, :].reshape(3, 4, 2, 8, 128).astype(BF16)

    to_up = pltpu.make_async_remote_copy(
        src_ref=ind.at[:, 3], dst_ref=low, send_sem=halo_send.at[0], recv_sem=halo_recv.at[0],
        device_id={"rad": up},
    )
    to_down = pltpu.make_async_remote_copy(
        src_ref=ind.at[:, 0], dst_ref=high, send_sem=halo_send.at[1], recv_sem=halo_recv.at[1],
        device_id={"rad": down},
    )
    to_up.start()
    to_down.start()

    for half in range(2):
        lanes = pl.ds(half * 128, 128)
        adv[:, :, :, :, lanes] = out[half, 0:192, :].reshape(3, 4, 2, 8, 128).astype(BF16)
    pltpu.make_async_copy(efin, efin, e_recv.at[1]).wait()
    for q in range(2):
        for s in range(4):
            for half in range(2):
                energy[q, s:s + 1, half * 128:(half + 1) * 128] = efin[(q * 4 + s) * 2 + half]

    shells = [ind[:, s].astype(F32) for s in range(4)]
    grad[:, 1] = ((shells[2] - shells[0]) * 0.5).astype(BF16)
    grad[:, 2] = ((shells[3] - shells[1]) * 0.5).astype(BF16)
    to_up.wait()
    to_down.wait()
    below = low[...].astype(F32) * jnp.where(my_rad == 0, 0.0, 1.0)
    above = high[...].astype(F32) * jnp.where(my_rad == RAD - 1, 0.0, 1.0)
    grad[:, 0] = ((shells[1] - below) * 0.5).astype(BF16)
    grad[:, 3] = ((above - shells[2]) * 0.5).astype(BF16)

    others = pl.ds(0, (HARM - 1) * 8)
    for k in range(3):
        sent = wire.at[k, :, others, :]
        pltpu.make_async_copy(sent, sent, mode_send.at[k]).wait()
    for part, tiles in ((0, tiles_a), (1, tiles_b)):
        sent = spec.at[tiles, others, :]
        pltpu.make_async_copy(sent, sent, spec_send.at[part]).wait()
    pltpu.make_async_copy(erecv.at[pl.ds(0, 31)], erecv.at[pl.ds(0, 31)], e_send.at[0]).wait()
    pltpu.make_async_copy(efin.at[pl.ds(0, 15)], efin.at[pl.ds(0, 15)], e_send.at[1]).wait()


def local(velocity, magnetic, vorticity, current):
    vmem = pl.BlockSpec(memory_space=pltpu.VMEM)
    block = velocity.shape
    return pl.pallas_call(
        kernel,
        out_shape=(
            jax.ShapeDtypeStruct(block, BF16),
            jax.ShapeDtypeStruct(block, BF16),
            jax.ShapeDtypeStruct((2, 4, L), F32),
        ),
        in_specs=[vmem] * 4,
        out_specs=(vmem,) * 3,
        scratch_shapes=[
            pltpu.VMEM((2, L * 8, 128), F32),
            pltpu.VMEM((8, 192, L), BF16),
            pltpu.VMEM((2, 768 + 2 * CROW, 128), F32),
            pltpu.VMEM((384, 512), BF16),
            pltpu.VMEM((3, 3, 256, 128), F32),
            pltpu.VMEM((3, 3, 256, 128), BF16),
            pltpu.VMEM((3, 3, 256, 128), BF16),
            pltpu.VMEM((2, 256, NPHI), BF16),
            pltpu.VMEM((384, 256), BF16),
            pltpu.VMEM((192, NPHI), F32),
            pltpu.VMEM((256, NPHI), BF16),
            pltpu.VMEM((5, 256, 128), BF16),
            pltpu.VMEM((5, 256, 128), BF16),
            pltpu.VMEM((5, 256, 128), F32),
            pltpu.VMEM((192, 256), BF16),
            pltpu.VMEM((2, 384, 128), F32),
            pltpu.VMEM((3, 4, 2, 8, L), BF16),
            pltpu.VMEM((3, 2, 8, L), BF16),
            pltpu.VMEM((3, 2, 8, L), BF16),
            pltpu.VMEM((16, 1, 128), F32),
            pltpu.VMEM((HARM, 1, 128), F32),
            pltpu.VMEM((1, 1, 128), F32),
            pltpu.VMEM((16, 1, 128), F32),
            pltpu.SemaphoreType.DMA((3,)),
            pltpu.SemaphoreType.DMA((3,)),
            pltpu.SemaphoreType.DMA((2,)),
            pltpu.SemaphoreType.DMA((2,)),
            pltpu.SemaphoreType.DMA((2,)),
            pltpu.SemaphoreType.DMA((2,)),
            pltpu.SemaphoreType.DMA((2,)),
            pltpu.SemaphoreType.DMA((2,)),
        ],
        compiler_params=pltpu.CompilerParams(collective_id=0, has_side_effects=True),
    )(velocity, magnetic, vorticity, current)


def solution(mesh):
    split = P(None, "rad", None, "harm", None)
    return jax.shard_map(
        local,
        mesh=mesh,
        in_specs=(split,) * 4,
        out_specs=(split, split, P(None, "rad", None)),
        check_vma=False,
    )
```

```python
import functools

import jax
import jax.numpy as jnp
from jax import lax
from jax.experimental import pallas as pl
from jax.experimental.pallas import tpu as pltpu
from jax.sharding import PartitionSpec as P

F32 = jnp.float32
BF16 = jnp.bfloat16
PI = 3.14159265358979
L = 256
HARM = 32
RAD = 16
NPHI = 768
GROUP = 4
CROW = 64


def sin_poly(y):
    z = y * y
    s = -1.0 / 39916800.0
    for c in (1.0 / 362880.0, -1.0 / 5040.0, 1.0 / 120.0, -1.0 / 6.0, 1.0):
        s = s * z + c
    return y * s


def cos_768(q):
    return sin_poly((192.0 - jnp.minimum(q, 768.0 - q)) * (PI / 384.0))


def mod_768(v):
    return v - 768.0 * jnp.floor((v + 0.5) * (1.0 / 768.0))


def iota(shape, dim):
    return lax.broadcasted_iota(jnp.int32, shape, dim)


def fiota(shape, dim):
    return iota(shape, dim).astype(F32)


def parity_sign(order):
    return 1.0 - 2.0 * ((iota((1, L), 1) + order) & 1).astype(F32)


def legendre_steps(me, tab):
    order = (me * 8 + iota((8, 128), 0)).astype(F32)
    order_sq = order * order
    degree = fiota((8, L), 1)
    own = (me * 8 + iota((8, L), 0)).astype(F32)
    logs = 0.5 * jnp.log((2.0 * degree + 1.0) / jnp.maximum(2.0 * degree, 1.0))
    taken = jnp.where((degree >= 1.0) & (degree <= own), logs, 0.0)
    log_start = 0.5 * jnp.log(jnp.full((8, 1), 0.5, F32)) + jnp.sum(taken, axis=1, keepdims=True)
    cosine, sector, unscale = [], [], []
    for jt in range(2):
        odd = 2.0 * (fiota((8, 128), 1) + 128.0 * jt) + 1.0
        cosine.append(sin_poly((384.0 - odd) * (PI / 768.0)))
        sine = sin_poly(jnp.minimum(odd, 768.0 - odd) * (PI / 768.0))
        log_sector = log_start + order * jnp.log(sine)
        sector.append(jnp.exp(jnp.maximum(log_sector, -60.0)))
        unscale.append(jnp.exp(jnp.minimum(log_sector + 60.0, 0.0)))
    zero = jnp.zeros((8, 128), F32)
    per = 16

    def block(index, state):
        q0, p0, q1, p1, back = state
        for inner in range(per):
            deg_i = index * per + inner
            deg = deg_i.astype(F32)
            sq = deg * deg
            live = order < deg
            t = (4.0 * sq - 1.0) / jnp.where(live, sq - order_sq, 1.0)
            a = jnp.where(live, jnp.sqrt(t), 0.0)
            ab = a * back
            back = jnp.where(live, lax.rsqrt(t), 0.0)
            start = order == deg
            n0 = a * cosine[0] * q0 + (jnp.where(start, sector[0], 0.0) - ab * p0)
            n1 = a * cosine[1] * q1 + (jnp.where(start, sector[1], 0.0) - ab * p1)
            row = pl.ds(pl.multiple_of(deg_i * 8, 8), 8)
            tab[0, row, :] = n0 * unscale[0]
            tab[1, row, :] = n1 * unscale[1]
            q0, p0, q1, p1 = n0, q0, n1, q1
        return q0, p0, q1, p1, back

    lax.fori_loop(0, L // per, block, (zero, zero, zero, zero, zero))


def kernel(
    vel, mag, vor, cur,
    adv, grad, energy,
    fields,
    tab, qt, coef, rhs, synth, wire, modes, trig, turned, grid, prod, spec, back, backf,
    acc, out, ind, low, high, esrc, erecv, ered, efin,
    field_sem, mode_send, mode_recv, spec_send, spec_recv, halo_send, halo_recv, e_send, e_recv,
):
    me = lax.axis_index("harm")
    my_rad = lax.axis_index("rad")
    up = lax.rem(my_rad + 1, RAD)
    down = lax.rem(my_rad + RAD - 1, RAD)

    def peer(i):
        return lax.rem(me + i, HARM)

    barrier = pltpu.get_barrier_semaphore()

    def greet(i, carry):
        pl.semaphore_signal(barrier, inc=1, device_id={"harm": peer(i)})
        return carry

    lax.fori_loop(1, HARM, greet, 0)
    pl.semaphore_signal(barrier, inc=1, device_id={"rad": up})
    pl.semaphore_signal(barrier, inc=1, device_id={"rad": down})

    arrivals = [
        pltpu.make_async_copy(ref, fields.at[a], field_sem.at[a])
        for a, ref in enumerate((vel, mag, vor, cur))
    ]
    for arrival in arrivals:
        arrival.start()

    legendre_steps(me, tab)

    coef[:, 0:CROW, :] = jnp.zeros((2, CROW, 128), F32)
    coef[:, CROW + 768:, :] = jnp.zeros((2, CROW, 128), F32)
    for a, arrival in enumerate(arrivals):
        arrival.wait()
        for half in range(2):
            lanes = pl.ds(half * 128, 128)
            coef[half, CROW + 192 * a:CROW + 192 * (a + 1), :] = (
                fields[a, :, :, :, :, lanes].astype(F32).reshape(192, 128)
            )

    row8 = iota((8, 128), 0)

    def synthesis(m, slot):
        for jt, rows in ((0, 128), (1, 64)):
            table = tab[jt, pl.ds(m, L, stride=8), :]
            qt[m, jt * 128:jt * 128 + rows, :] = table.T[0:rows].astype(BF16)
        sign = parity_sign(m)
        for r in range(2):
            for half in range(2):
                sgn = sign[:, half * 128:(half + 1) * 128]
                before = None
                for c in range(-1, 12):
                    rows = coef[half, pl.ds(CROW + c * 64 + r * 8 + m, 8, stride=16), :]
                    if c >= 0:
                        base = r * 192 + c * 16
                        for gn, part in ((0, jnp.where(row8 < 4, rows, 0.0)),
                                         (1, jnp.where(row8 >= 4, before, 0.0))):
                            lane = gn * 256 + half * 128
                            rhs[slot, base:base + 16, lane:lane + 128] = jnp.concatenate(
                                [part, part * sgn], axis=0
                            ).astype(BF16)
                    before = rows
        lhs = jnp.concatenate([qt[m, 0:96, :], qt[m, 96:192, :]], axis=1)
        made = lax.dot_general(
            lhs, rhs[slot], (((1,), (1,)), ((), ())), preferred_element_type=F32
        ) * (1.0 / L)
        for k in range(3):
            for lt in range(3):
                synth[k, lt, pl.ds(m, 32, stride=8), :] = made[
                    k * 32:(k + 1) * 32, lt * 128:(lt + 1) * 128
                ]

    def synthesis_group(group, carry):
        for inner in range(GROUP):
            synthesis(group * GROUP + inner, inner)
        return carry

    lax.fori_loop(0, 8 // GROUP, synthesis_group, 0)
    wire[...] = synth[...].astype(BF16)

    pl.semaphore_wait(barrier, HARM + 1)

    def rows_of(device):
        return pl.ds(pl.multiple_of(device * 8, 8), 8)

    def mode_copy(k, i):
        to = peer(i)
        return pltpu.make_async_remote_copy(
            src_ref=wire.at[k, :, rows_of(to), :],
            dst_ref=modes.at[k, :, rows_of(me), :],
            send_sem=mode_send.at[k],
            recv_sem=mode_recv.at[k],
            device_id={"harm": to},
        )

    for k in range(3):
        def send_modes(i, carry, k=k):
            mode_copy(k, i).start()
            return carry

        lax.fori_loop(1, HARM, send_modes, 0)
        pltpu.make_async_copy(
            wire.at[k, :, rows_of(me), :], modes.at[k, :, rows_of(me), :], mode_recv.at[k]
        ).start()

    order8 = me * 8 + iota((8, 128), 0)
    for half in range(2):
        degree = iota((8, 128), 1) + 128 * half
        weight = jnp.where(degree >= order8, 1.0 / (2.0 * degree.astype(F32) + 1.0), 0.0)
        weights = (
            weight * jnp.where(order8 == 0, 0.5, 1.0),
            weight * jnp.where(order8 == 0, 0.0, 1.0),
        )
        for q in range(2):
            for s in range(4):
                total = jnp.zeros((8, 128), F32)
                for c in range(3):
                    for r in range(2):
                        at = CROW + (((q * 3 + c) * 4 + s) * 2 + r) * 8
                        value = coef[half, at:at + 8, :]
                        total += value * value * weights[r]
                esrc[(q * 4 + s) * 2 + half] = jnp.sum(total, axis=0, keepdims=True)

    def energy_copy(i):
        to = peer(i)
        return pltpu.make_async_remote_copy(
            src_ref=esrc.at[lax.rem(to, 16)],
            dst_ref=erecv.at[me],
            send_sem=e_send.at[0],
            recv_sem=e_recv.at[0],
            device_id={"harm": to},
        )

    def send_energy(i, carry):
        energy_copy(i).start()
        return carry

    lax.fori_loop(1, HARM, send_energy, 0)
    pltpu.make_async_copy(esrc.at[lax.rem(me, 16)], erecv.at[me], e_recv.at[0]).start()

    def trig_rows(b, carry):
        angle = mod_768((b * 8 + iota((8, NPHI), 0)).astype(F32) * fiota((8, NPHI), 1))
        rows = pl.ds(pl.multiple_of(b * 8, 8), 8)
        trig[0, rows, :] = cos_768(angle).astype(BF16)
        trig[1, rows, :] = cos_768(jnp.where(angle >= 192.0, angle - 192.0, angle + 576.0)).astype(BF16)
        return carry

    lax.fori_loop(0, 32, trig_rows, 0)

    lane = iota((1, 128), 1)
    factors = []
    for k in range(3):
        row = ((lane >> 2) & 1) * 96 + k * 32 + me
        wave = fiota((192, 128), 0) + 1.0
        odd = (2 * row + 1).astype(F32)
        series = cos_768(mod_768(wave * odd)) / (4.0 * wave * wave - 1.0)
        weight = (2.0 / 384.0) * (1.0 - 2.0 * jnp.sum(series, axis=0, keepdims=True))
        factors.append(weight * (256.0 / 768.0))

    def grid_of(k):
        for lt in range(3):
            turned[lt * 128:(lt + 1) * 128, :] = modes[k, lt].T
        grid[...] = jnp.dot(turned[0:192], trig[0], preferred_element_type=F32) + jnp.dot(
            turned[192:384], trig[1], preferred_element_type=F32
        )
        for pt in range(6):
            cols = slice(pt * 128, (pt + 1) * 128)
            g = [grid[c * 16:(c + 1) * 16, cols] for c in range(12)]
            u, b, w, j = g[0:3], g[3:6], g[6:9], g[9:12]

            def cross(x, y, i):
                n, o = (i + 1) % 3, (i + 2) % 3
                return x[n] * y[o] - x[o] * y[n]

            for c in range(6):
                value = cross(u, w, c) + cross(j, b, c) if c < 3 else cross(u, b, c - 3)
                value = value.astype(BF16)
                base = 96 + c * 16 if c < 3 else (c - 3) * 16
                for at in (base, base + 48):
                    prod[at:at + 16, cols] = value
                    if at >= 128:
                        prod[at + 64:at + 80, cols] = value

    mode_weight = jnp.where(iota((256, 1), 0) == 0, 1.0, 2.0)
    near = iota((1, 128), 1)
    take_cosine = (
        (near < 48) | (near >= 96),
        (near & 63) < 16,
    )

    def analysed(k):
        cosine, sine = (
            lax.dot_general(
                trig[r], prod[...], (((1,), (1,)), ((), ())), preferred_element_type=F32
            )
            for r in range(2)
        )
        scale = mode_weight * factors[k]
        return [
            jnp.where(take_cosine[t], cosine[:, t * 128:t * 128 + 128], sine[:, t * 128:t * 128 + 128])
            * scale
            for t in range(2)
        ]

    def wait_modes(k):
        pltpu.make_async_copy(modes.at[k], modes.at[k], mode_recv.at[k]).wait()

    def spec_copy(part, i):
        to, tiles = peer(i), parts[part]
        return pltpu.make_async_remote_copy(
            src_ref=spec.at[tiles, rows_of(to), :],
            dst_ref=back.at[tiles, rows_of(me), :],
            send_sem=spec_send.at[part],
            recv_sem=spec_recv.at[part],
            device_id={"harm": to},
        )

    def send_spectra(part):
        tiles = parts[part]

        def one(i, carry):
            spec_copy(part, i).start()
            return carry

        lax.fori_loop(1, HARM, one, 0)
        pltpu.make_async_copy(
            spec.at[tiles, rows_of(me), :], back.at[tiles, rows_of(me), :], spec_recv.at[part]
        ).start()

    parts = (pl.ds(0, 2), pl.ds(2, 1), pl.ds(3, 2))
    wait_modes(0)
    grid_of(0)
    lead, trail0 = analysed(0)
    spec[0] = lead.astype(BF16)
    wait_modes(1)
    grid_of(1)
    lead, trail1 = analysed(1)
    spec[1] = lead.astype(BF16)
    send_spectra(0)
    spec[3] = jnp.where(near < 64, trail0, trail1).astype(BF16)

    pltpu.make_async_copy(erecv, erecv, e_recv.at[0]).wait()
    ered[...] = jnp.sum(erecv[...], axis=0, keepdims=True)
    mine = lax.rem(me, 16)

    def row_copy(i):
        to = me - mine + lax.rem(mine + i, 16)
        return pltpu.make_async_remote_copy(
            src_ref=ered.at[0],
            dst_ref=efin.at[mine],
            send_sem=e_send.at[1],
            recv_sem=e_recv.at[1],
            device_id={"harm": to},
        )

    def send_row(i, carry):
        row_copy(i).start()
        return carry

    lax.fori_loop(1, 16, send_row, 0)
    pltpu.make_async_copy(ered.at[0], efin.at[mine], e_recv.at[1]).start()

    wait_modes(2)
    grid_of(2)
    lead, trail = analysed(2)
    spec[2] = lead.astype(BF16)
    send_spectra(1)
    spec[4] = trail.astype(BF16)
    send_spectra(2)

    def wait_spectra(part):
        tiles = parts[part]
        pltpu.make_async_copy(back.at[tiles], back.at[tiles], spec_recv.at[part]).wait()
        backf[tiles] = back[tiles].astype(F32)

    lane_row = iota((32, 128), 1)
    gn_of = (lane_row >> 2) & 1

    def split(rows):
        return jnp.concatenate(
            [jnp.where(gn_of == gn, part, 0.0) for gn in range(2) for part in rows], axis=0
        ).astype(BF16)

    def column(tile, m):
        return backf[tile, pl.ds(m, 32, stride=8), :]

    def table(m, ks):
        return jnp.concatenate(
            [qt[m, gn * 96 + ks[0] * 32:gn * 96 + ks[-1] * 32 + 32, :] for gn in range(2)], axis=0
        )

    def over_rows(values, m, ks):
        return lax.dot_general(
            split(values), table(m, ks), (((0,), (0,)), ((), ())), preferred_element_type=F32
        )

    def store(sums, at, kind, r, c, m):
        sign = parity_sign(m)
        both = sums[at:at + 8] + sums[at + 8:at + 16] * sign
        both = both[0:4] + both[4:8]
        for half in range(2):
            out[half, pl.ds(kind * 192 + c * 64 + r * 8 + m, 4, stride=16), :] = both[
                :, half * 128:(half + 1) * 128
            ]

    wait_spectra(0)
    for m in range(8):
        acc[m] = over_rows([column(0, m), column(1, m)], m, (0, 1))
    wait_spectra(1)
    for m in range(8):
        sums = acc[m] + over_rows([column(2, m)], m, (2,))
        for r in range(2):
            for c in range(3):
                store(sums, r * 48 + c * 16, 1, r, c, m)
        for c in range(2):
            store(sums, 96 + c * 16, 0, 0, c, m)

    for half in range(2):
        lanes = pl.ds(half * 128, 128)
        ind[:, :, :, :, lanes] = out[half, 192:384, :].reshape(3, 4, 2, 8, 128).astype(BF16)

    to_up = pltpu.make_async_remote_copy(
        src_ref=ind.at[:, 3], dst_ref=low, send_sem=halo_send.at[0], recv_sem=halo_recv.at[0],
        device_id={"rad": up},
    )
    to_down = pltpu.make_async_remote_copy(
        src_ref=ind.at[:, 0], dst_ref=high, send_sem=halo_send.at[1], recv_sem=halo_recv.at[1],
        device_id={"rad": down},
    )
    to_up.start()
    to_down.start()

    wait_spectra(2)
    for m in range(8):
        pair, last = column(3, m), column(4, m)
        sums = over_rows(
            [
                jnp.where(lane_row < 64, pair, 0.0),
                jnp.where(lane_row >= 64, pair, 0.0),
                jnp.where(lane_row < 64, last, 0.0),
            ],
            m, (0, 1, 2),
        )
        sums = sums[0:64] + sums[64:128]
        store(sums, 0, 0, 0, 2, m)
        for c in range(3):
            store(sums, 16 + c * 16, 0, 1, c, m)

    for half in range(2):
        lanes = pl.ds(half * 128, 128)
        adv[:, :, :, :, lanes] = out[half, 0:192, :].reshape(3, 4, 2, 8, 128).astype(BF16)
    pltpu.make_async_copy(efin, efin, e_recv.at[1]).wait()
    for q in range(2):
        for s in range(4):
            for half in range(2):
                energy[q, s:s + 1, half * 128:(half + 1) * 128] = efin[(q * 4 + s) * 2 + half]

    shells = [ind[:, s].astype(F32) for s in range(4)]
    grad[:, 1] = ((shells[2] - shells[0]) * 0.5).astype(BF16)
    grad[:, 2] = ((shells[3] - shells[1]) * 0.5).astype(BF16)
    to_up.wait()
    to_down.wait()
    below = low[...].astype(F32) * jnp.where(my_rad == 0, 0.0, 1.0)
    above = high[...].astype(F32) * jnp.where(my_rad == RAD - 1, 0.0, 1.0)
    grad[:, 0] = ((shells[1] - below) * 0.5).astype(BF16)
    grad[:, 3] = ((above - shells[2]) * 0.5).astype(BF16)

    others = pl.ds(0, (HARM - 1) * 8)
    for k in range(3):
        sent = wire.at[k, :, others, :]
        pltpu.make_async_copy(sent, sent, mode_send.at[k]).wait()
    for part in range(3):
        sent = spec.at[parts[part], others, :]
        pltpu.make_async_copy(sent, sent, spec_send.at[part]).wait()
    pltpu.make_async_copy(erecv.at[pl.ds(0, 31)], erecv.at[pl.ds(0, 31)], e_send.at[0]).wait()
    pltpu.make_async_copy(efin.at[pl.ds(0, 15)], efin.at[pl.ds(0, 15)], e_send.at[1]).wait()


def local(velocity, magnetic, vorticity, current):
    vmem = pl.BlockSpec(memory_space=pltpu.VMEM)
    block = velocity.shape
    return pl.pallas_call(
        kernel,
        out_shape=(
            jax.ShapeDtypeStruct(block, BF16),
            jax.ShapeDtypeStruct(block, BF16),
            jax.ShapeDtypeStruct((2, 4, L), F32),
        ),
        in_specs=[pl.BlockSpec(memory_space=pl.ANY)] * 4,
        out_specs=(vmem,) * 3,
        scratch_shapes=[
            pltpu.VMEM((4,) + block, BF16),
            pltpu.VMEM((2, L * 8, 128), F32),
            pltpu.VMEM((8, 192, L), BF16),
            pltpu.VMEM((2, 768 + 2 * CROW, 128), F32),
            pltpu.VMEM((GROUP, 384, 512), BF16),
            pltpu.VMEM((3, 3, 256, 128), F32),
            pltpu.VMEM((3, 3, 256, 128), BF16),
            pltpu.VMEM((3, 3, 256, 128), BF16),
            pltpu.VMEM((2, 256, NPHI), BF16),
            pltpu.VMEM((384, 256), BF16),
            pltpu.VMEM((192, NPHI), F32),
            pltpu.VMEM((256, NPHI), BF16),
            pltpu.VMEM((5, 256, 128), BF16),
            pltpu.VMEM((5, 256, 128), BF16),
            pltpu.VMEM((5, 256, 128), F32),
            pltpu.VMEM((8, 128, L), F32),
            pltpu.VMEM((2, 384, 128), F32),
            pltpu.VMEM((3, 4, 2, 8, L), BF16),
            pltpu.VMEM((3, 2, 8, L), BF16),
            pltpu.VMEM((3, 2, 8, L), BF16),
            pltpu.VMEM((16, 1, 128), F32),
            pltpu.VMEM((HARM, 1, 128), F32),
            pltpu.VMEM((1, 1, 128), F32),
            pltpu.VMEM((16, 1, 128), F32),
            pltpu.SemaphoreType.DMA((4,)),
            pltpu.SemaphoreType.DMA((3,)),
            pltpu.SemaphoreType.DMA((3,)),
            pltpu.SemaphoreType.DMA((3,)),
            pltpu.SemaphoreType.DMA((3,)),
            pltpu.SemaphoreType.DMA((2,)),
            pltpu.SemaphoreType.DMA((2,)),
            pltpu.SemaphoreType.DMA((2,)),
            pltpu.SemaphoreType.DMA((2,)),
        ],
        compiler_params=pltpu.CompilerParams(collective_id=0, has_side_effects=True),
    )(velocity, magnetic, vorticity, current)


def solution(mesh):
    split = P(None, "rad", None, "harm", None)
    return jax.shard_map(
        local,
        mesh=mesh,
        in_specs=(split,) * 4,
        out_specs=(split, split, P(None, "rad", None)),
        check_vma=False,
    )
```

```python
import jax
import jax.numpy as jnp
from jax import lax
from jax.experimental import pallas as pl
from jax.experimental.pallas import tpu as pltpu
from jax.sharding import PartitionSpec as P

F32 = jnp.float32
BF16 = jnp.bfloat16
PI = 3.14159265358979
L = 256
HARM = 32
RAD = 16
NPHI = 768
GROUP = 4

PAIRS = ((0, 3), (1, 2))
EARLY = [(c, 0) for c in range(8)]
LATER = [(c, 0) for c in range(8, 12)] + [(c, 1) for c in range(12)]
SLOT_ROW = {}
for at, (c, pair) in enumerate(EARLY):
    for r in range(2):
        SLOT_ROW[c, pair, r] = r * 64 + at * 8
for at, (c, pair) in enumerate(LATER):
    for r in range(2):
        SLOT_ROW[c, pair, r] = 128 + r * 128 + at * 8
ROW_SLOT = {row: slot for slot, row in SLOT_ROW.items()}


def sin_poly(y):
    z = y * y
    s = -1.0 / 39916800.0
    for c in (1.0 / 362880.0, -1.0 / 5040.0, 1.0 / 120.0, -1.0 / 6.0, 1.0):
        s = s * z + c
    return y * s


def cos_768(q):
    return sin_poly((192.0 - jnp.minimum(q, 768.0 - q)) * (PI / 384.0))


def mod_768(v):
    return v - 768.0 * jnp.floor((v + 0.5) * (1.0 / 768.0))


def iota(shape, dim):
    return lax.broadcasted_iota(jnp.int32, shape, dim)


def fiota(shape, dim):
    return iota(shape, dim).astype(F32)


def parity_sign(order, rows=1):
    return 1.0 - 2.0 * ((iota((rows, L), 1) + order) & 1).astype(F32)


def dot_nt(a, b):
    return lax.dot_general(a, b, (((1,), (1,)), ((), ())), preferred_element_type=F32)


def dot_tn(a, b):
    return lax.dot_general(a, b, (((0,), (0,)), ((), ())), preferred_element_type=F32)


def legendre_steps(me, tab):
    order = (me * 8 + iota((8, 128), 0)).astype(F32)
    order_sq = order * order
    degree = fiota((8, L), 1)
    own = (me * 8 + iota((8, L), 0)).astype(F32)
    logs = 0.5 * jnp.log((2.0 * degree + 1.0) / jnp.maximum(2.0 * degree, 1.0))
    taken = jnp.where((degree >= 1.0) & (degree <= own), logs, 0.0)
    log_start = 0.5 * jnp.log(jnp.full((8, 1), 0.5, F32)) + jnp.sum(taken, axis=1, keepdims=True)
    cosine, sector, unscale = [], [], []
    for jt in range(2):
        odd = 2.0 * (fiota((8, 128), 1) + 128.0 * jt) + 1.0
        cosine.append(sin_poly((384.0 - odd) * (PI / 768.0)))
        sine = sin_poly(jnp.minimum(odd, 768.0 - odd) * (PI / 768.0))
        log_sector = log_start + order * jnp.log(sine)
        sector.append(jnp.exp(jnp.maximum(log_sector, -60.0)))
        unscale.append(jnp.exp(jnp.minimum(log_sector + 60.0, 0.0)))
    zero = jnp.zeros((8, 128), F32)
    per = 16

    def block(index, state):
        q0, p0, q1, p1, back = state
        for inner in range(per):
            deg_i = index * per + inner
            deg = deg_i.astype(F32)
            sq = deg * deg
            live = order < deg
            t = (4.0 * sq - 1.0) / jnp.where(live, sq - order_sq, 1.0)
            a = jnp.where(live, jnp.sqrt(t), 0.0)
            ab = a * back
            back = jnp.where(live, lax.rsqrt(t), 0.0)
            start = order == deg
            n0 = a * cosine[0] * q0 + (jnp.where(start, sector[0], 0.0) - ab * p0)
            n1 = a * cosine[1] * q1 + (jnp.where(start, sector[1], 0.0) - ab * p1)
            row = pl.ds(pl.multiple_of(deg_i * 8, 8), 8)
            tab[0, row, :] = n0 * unscale[0]
            tab[1, row, :] = n1 * unscale[1]
            q0, p0, q1, p1 = n0, q0, n1, q1
        return q0, p0, q1, p1, back

    lax.fori_loop(0, L // per, block, (zero, zero, zero, zero, zero))


def kernel(
    vel, mag, vor, cur,
    adv, grad, energy,
    fields,
    tab, qt, coef, rhs, synth, wire, modes, trig, turned, turned_early, grid, grid_early,
    prod, prod_early, spec, back, backf,
    acc, out, ind, low, high, esrc, erecv, ered, efin,
    field_sem, mode_send, mode_recv, spec_send, spec_recv, halo_send, halo_recv, e_send, e_recv,
):
    me = lax.axis_index("harm")
    my_rad = lax.axis_index("rad")
    above = my_rad < RAD - 1
    below = my_rad > 0

    def peer(i):
        return lax.rem(me + i, HARM)

    barrier = pltpu.get_barrier_semaphore()

    def greet(i, carry):
        pl.semaphore_signal(barrier, inc=1, device_id={"harm": peer(i)})
        return carry

    lax.fori_loop(1, HARM, greet, 0)

    @pl.when(above)
    def _():
        pl.semaphore_signal(barrier, inc=1, device_id={"rad": my_rad + 1})

    @pl.when(below)
    def _():
        pl.semaphore_signal(barrier, inc=1, device_id={"rad": my_rad - 1})

    arrivals = [
        pltpu.make_async_copy(ref, fields.at[a], field_sem.at[a])
        for a, ref in enumerate((vel, mag, vor, cur))
    ]
    for arrival in arrivals:
        arrival.start()

    @pl.when(jnp.logical_not(below))
    def _():
        low[...] = jnp.zeros(low.shape, BF16)

    @pl.when(jnp.logical_not(above))
    def _():
        high[...] = jnp.zeros(high.shape, BF16)

    legendre_steps(me, tab)

    for a, arrival in enumerate(arrivals):
        arrival.wait()
        for c in range(3):
            for r in range(2):
                for pair in range(2):
                    both = fields[a, c, PAIRS[pair][0], r], fields[a, c, PAIRS[pair][1], r]
                    both = jnp.concatenate([v.astype(F32) for v in both], axis=0)
                    at = ((r * 12 + a * 3 + c) * 2 + pair) * 64
                    for half in range(2):
                        part = both[:, half * 128:(half + 1) * 128]
                        for copy in range(4):
                            coef[half, at + copy * 16:at + copy * 16 + 16, :] = part

    slot_row = iota((8, 128), 0)

    def synthesis(m, slot):
        for jt, rows in ((0, 128), (1, 64)):
            table = tab[jt, pl.ds(m, L, stride=8), :]
            qt[m, jt * 128:jt * 128 + rows, :] = table.T[0:rows].astype(BF16)
        sign = parity_sign(m, 8)
        for half in range(2):
            sgn = jnp.where(slot_row >= 4, sign[:, half * 128:(half + 1) * 128], 1.0)
            keep = [jnp.where(((slot_row >> 1) & 1) == gn, sgn, 0.0) for gn in range(2)]
            for row in range(0, 384, 16):
                values = []
                for at in (row, row + 8):
                    c, pair, r = ROW_SLOT[at]
                    first = ((r * 12 + c) * 2 + pair) * 64
                    values.append(coef[half, pl.ds(first + m, 8, stride=8), :])
                for gn in range(2):
                    lane = gn * 256 + half * 128
                    rhs[slot, row:row + 16, lane:lane + 128] = jnp.concatenate(
                        [v * keep[gn] for v in values], axis=0
                    ).astype(BF16)
        lhs = jnp.concatenate([qt[m, 0:96, :], qt[m, 96:192, :]], axis=1)
        made = dot_nt(lhs, rhs[slot]) * (1.0 / L)
        for k in range(3):
            for lt in range(3):
                synth[k, lt, pl.ds(m, 32, stride=8), :] = made[
                    k * 32:(k + 1) * 32, lt * 128:(lt + 1) * 128
                ]

    def synthesis_group(group, carry):
        for inner in range(GROUP):
            synthesis(group * GROUP + inner, inner)
        return carry

    lax.fori_loop(0, 8 // GROUP, synthesis_group, 0)
    wire[...] = synth[...].astype(BF16)

    pl.semaphore_wait(barrier, HARM - 1 + above.astype(jnp.int32) + below.astype(jnp.int32))

    def rows_of(device):
        return pl.ds(pl.multiple_of(device * 8, 8), 8)

    def mode_part(ref, group, rows):
        if group == 0:
            return ref.at[:, 0, rows, :]
        return ref.at[group - 1, pl.ds(1, 2), rows, :]

    def send_modes(group):
        def one(i, carry):
            to = peer(i)
            pltpu.make_async_remote_copy(
                src_ref=mode_part(wire, group, rows_of(to)),
                dst_ref=mode_part(modes, group, rows_of(me)),
                send_sem=mode_send.at[group],
                recv_sem=mode_recv.at[group],
                device_id={"harm": to},
            ).start()
            return carry

        lax.fori_loop(1, HARM, one, 0)
        pltpu.make_async_copy(
            mode_part(wire, group, rows_of(me)),
            mode_part(modes, group, rows_of(me)),
            mode_recv.at[group],
        ).start()

    def wait_modes(group):
        landed = mode_part(modes, group, pl.ds(0, 256))
        pltpu.make_async_copy(landed, landed, mode_recv.at[group]).wait()

    send_modes(0)
    send_modes(1)

    order8 = me * 8 + iota((8, 128), 0)
    for half in range(2):
        degree = iota((8, 128), 1) + 128 * half
        weight = jnp.where(degree >= order8, 1.0 / (2.0 * degree.astype(F32) + 1.0), 0.0)
        weights = (
            weight * jnp.where(order8 == 0, 0.5, 1.0),
            weight * jnp.where(order8 == 0, 0.0, 1.0),
        )
        for q in range(2):
            for s in range(4):
                pair = 0 if s in PAIRS[0] else 1
                total = jnp.zeros((8, 128), F32)
                for c in range(3):
                    for r in range(2):
                        at = ((r * 12 + q * 3 + c) * 2 + pair) * 64 + PAIRS[pair].index(s) * 8
                        value = coef[half, at:at + 8, :]
                        total += value * value * weights[r]
                esrc[(q * 4 + s) * 2 + half] = jnp.sum(total, axis=0, keepdims=True)

    def send_energy(i, carry):
        to = peer(i)
        pltpu.make_async_remote_copy(
            src_ref=esrc.at[lax.rem(to, 16)],
            dst_ref=erecv.at[me],
            send_sem=e_send.at[0],
            recv_sem=e_recv.at[0],
            device_id={"harm": to},
        ).start()
        return carry

    lax.fori_loop(1, HARM, send_energy, 0)
    pltpu.make_async_copy(esrc.at[lax.rem(me, 16)], erecv.at[me], e_recv.at[0]).start()

    def trig_rows(b, carry):
        angle = mod_768((b * 8 + iota((8, NPHI), 0)).astype(F32) * fiota((8, NPHI), 1))
        rows = pl.ds(pl.multiple_of(b * 8, 8), 8)
        trig[0, rows, :] = cos_768(angle).astype(BF16)
        trig[1, rows, :] = cos_768(jnp.where(angle >= 192.0, angle - 192.0, angle + 576.0)).astype(BF16)
        return carry

    lax.fori_loop(0, 32, trig_rows, 0)

    lane = iota((1, 128), 1)
    factors = []
    for k in range(3):
        row = ((lane >> 1) & 1) * 96 + k * 32 + me
        wave = fiota((192, 128), 0) + 1.0
        odd = (2 * row + 1).astype(F32)
        series = cos_768(mod_768(wave * odd)) / (4.0 * wave * wave - 1.0)
        weight = (2.0 / 384.0) * (1.0 - 2.0 * jnp.sum(series, axis=0, keepdims=True))
        factors.append(weight * (256.0 / 768.0))
    mixed = jnp.where(lane < 32, factors[0], jnp.where(lane < 64, factors[1], factors[2]))
    mode_weight = jnp.where(iota((256, 1), 0) == 0, 1.0, 2.0)
    prod[:, 128:256, :] = jnp.zeros((3, 128, NPHI), BF16)
    prod_early[96:128, :] = jnp.zeros((32, NPHI), BF16)

    def cross(x, y, i):
        n, o = (i + 1) % 3, (i + 2) % 3
        return x[n] * y[o] - x[o] * y[n]

    def rounded_pair(first, second):
        return jnp.concatenate([first, second], axis=0).astype(BF16)

    def send_spectra(group):
        def one(i, carry):
            to = peer(i)
            pltpu.make_async_remote_copy(
                src_ref=spec.at[group, rows_of(to), :],
                dst_ref=back.at[group, rows_of(me), :],
                send_sem=spec_send.at[group],
                recv_sem=spec_recv.at[group],
                device_id={"harm": to},
            ).start()
            return carry

        lax.fori_loop(1, HARM, one, 0)
        pltpu.make_async_copy(
            spec.at[group, rows_of(me), :], back.at[group, rows_of(me), :], spec_recv.at[group]
        ).start()

    def wait_spectra(group):
        pltpu.make_async_copy(back.at[group], back.at[group], spec_recv.at[group]).wait()
        backf[group] = back[group].astype(F32)

    wait_modes(0)
    for k in range(3):
        turned_early[k] = modes[k, 0].T
    grid_early[...] = sum(
        jnp.dot(
            jnp.concatenate([turned_early[k, r * 64:(r + 1) * 64] for k in range(3)], axis=0),
            trig[r], preferred_element_type=F32,
        )
        for r in range(2)
    )
    even_row = (iota((8, 128), 0) & 1) == 0
    for k in range(3):
        for pt in range(6):
            cols = slice(pt * 128, (pt + 1) * 128)
            g = [grid_early[k * 64 + c * 8:k * 64 + c * 8 + 8, cols] for c in range(6)]
            x, y, z = (cross(g[0:3], g[3:6], i) for i in range(3))
            lower = jnp.where(even_row, x, pltpu.roll(y, 1, 0))
            upper = jnp.where(even_row, pltpu.roll(x, 7, 0), y).astype(BF16)
            pair = rounded_pair(lower, z)
            for r in range(2):
                prod_early[k * 32 + r * 16:k * 32 + r * 16 + 16, cols] = pair
                prod[k, r * 32:r * 32 + 8, cols] = upper
    early_c, early_s = (dot_nt(trig[r], prod_early[...]) for r in range(2))
    spec[0] = (
        jnp.where(((lane >> 4) & 1) == 0, early_c, early_s) * (mode_weight * mixed)
    ).astype(BF16)
    send_spectra(0)
    send_modes(2)
    send_modes(3)

    def later(k):
        for lt in range(2):
            turned[lt * 128:(lt + 1) * 128, :] = modes[k, 1 + lt].T
        grid[...] = sum(
            jnp.dot(turned[r * 128:(r + 1) * 128], trig[r], preferred_element_type=F32)
            for r in range(2)
        )
        for pt in range(6):
            cols = slice(pt * 128, (pt + 1) * 128)

            def value(c, pair):
                if pair == 0 and c < 8:
                    return grid_early[k * 64 + c * 8:k * 64 + c * 8 + 8, cols]
                at = (c - 8) * 8 if pair == 0 else 32 + c * 8
                return grid[at:at + 8, cols]

            u, b, w, j = ([value(v * 3 + i, 1) for i in range(3)] for v in range(4))
            inner = [cross(u, w, i) + cross(j, b, i) for i in range(3)]
            curl = [cross(u, b, i) for i in range(3)]
            u, b, w, j = ([value(v * 3 + i, 0) for i in range(3)] for v in range(4))
            ends = [cross(u, w, i) + cross(j, b, i) for i in range(3)]
            for r in range(2):
                prod[k, r * 32 + 8:r * 32 + 16, cols] = curl[0].astype(BF16)
                prod[k, r * 32 + 16:r * 32 + 32, cols] = rounded_pair(curl[1], curl[2])
                prod[k, 64 + r * 32:64 + r * 32 + 16, cols] = rounded_pair(ends[0], ends[1])
                prod[k, 80 + r * 32:80 + r * 32 + 16, cols] = rounded_pair(ends[2], inner[0])
                at = 128 + 32 * k + 16 * r
                prod[k, at:at + 16, cols] = rounded_pair(inner[1], inner[2])
        cosine, sine = (dot_nt(trig[r], prod[k]) for r in range(2))
        scale = mode_weight * factors[k]
        lead = jnp.where(((lane >> 5) & 1) == 0, cosine[:, 0:128], sine[:, 0:128]) * scale
        trail = jnp.where(((lane >> 4) & 1) == 0, cosine[:, 128:256], sine[:, 128:256]) * scale
        spec[1 + k] = lead.astype(BF16)
        return trail

    wait_modes(1)
    trail = later(0)
    send_spectra(1)

    col = iota((32, 128), 1)
    col_gn = (col >> 1) & 1

    def column(tile, m):
        return backf[tile, pl.ds(m, 32, stride=8), :]

    def table(m, ks):
        return jnp.concatenate(
            [qt[m, gn * 96 + ks[0] * 32:gn * 96 + ks[-1] * 32 + 32, :] for gn in range(2)], axis=0
        )

    def over_rows(values, m, ks):
        kept = jnp.concatenate(
            [jnp.where(col_gn == gn, part, 0.0) for gn in range(2) for part in values], axis=0
        ).astype(BF16)
        return dot_tn(kept, table(m, ks))

    def over_mixed(tile, m):
        values = column(tile, m)
        sums = over_rows(
            [jnp.where((col >> 5) == k, values, 0.0) for k in range(3)], m, (0, 1, 2)
        )
        return sums[0:32] + sums[32:64] + sums[64:96]

    lower_half = iota((8, L), 0) < 4

    def store(sums, at, row, stride, m):
        v = sums[at:at + 8] * jnp.where(lower_half, 1.0, parity_sign(m, 8))
        v = v + pltpu.roll(v, 4, 0)
        v = v + pltpu.roll(v, 6, 0)
        for half in range(2):
            out[half, pl.ds(row + m, 2, stride=stride), :] = v[0:2, half * 128:(half + 1) * 128]

    def keep_induction(s):
        for c in range(3):
            for half in range(2):
                rows = 192 + c * 64 + s * 16
                lanes = pl.ds(half * 128, 128)
                ind[c, s, :, :, lanes] = out[half, rows:rows + 16, :].reshape(2, 8, 128).astype(BF16)

    def halo_down():
        return pltpu.make_async_remote_copy(
            src_ref=ind.at[:, 0], dst_ref=high, send_sem=halo_send.at[1], recv_sem=halo_recv.at[1],
            device_id={"rad": my_rad - 1},
        )

    def halo_up():
        return pltpu.make_async_remote_copy(
            src_ref=ind.at[:, 3], dst_ref=low, send_sem=halo_send.at[0], recv_sem=halo_recv.at[0],
            device_id={"rad": my_rad + 1},
        )

    wait_spectra(0)
    for m in range(8):
        sums = over_mixed(0, m)
        for r in range(2):
            store(sums, r * 16, 192 + r * 8, 64, m)
            store(sums, r * 16 + 8, 192 + 128 + r * 8, 48, m)
    keep_induction(0)

    @pl.when(below)
    def _():
        halo_down().start()

    wait_modes(2)
    trail = jnp.where((lane >> 5) == 1, later(1), trail)
    send_spectra(2)

    pltpu.make_async_copy(erecv, erecv, e_recv.at[0]).wait()
    ered[...] = jnp.sum(erecv[...], axis=0, keepdims=True)
    mine = lax.rem(me, 16)

    def send_row(i, carry):
        pltpu.make_async_remote_copy(
            src_ref=ered.at[0],
            dst_ref=efin.at[mine],
            send_sem=e_send.at[1],
            recv_sem=e_recv.at[1],
            device_id={"harm": me - mine + lax.rem(mine + i, 16)},
        ).start()
        return carry

    lax.fori_loop(1, 16, send_row, 0)
    pltpu.make_async_copy(ered.at[0], efin.at[mine], e_recv.at[1]).start()

    wait_modes(3)
    trail = jnp.where((lane >> 5) == 2, later(2), trail)
    send_spectra(3)
    spec[4] = trail.astype(BF16)
    send_spectra(4)

    wait_spectra(1)
    wait_spectra(2)
    for m in range(8):
        acc[m] = over_rows([column(1, m), column(2, m)], m, (0, 1))
    wait_spectra(3)
    for m in range(8):
        sums = acc[m] + over_rows([column(3, m)], m, (2,))
        for r in range(2):
            store(sums, r * 32, 192 + 48 + r * 8, 64, m)
            for c in range(3):
                store(sums, r * 32 + 8 + c * 8, 192 + c * 64 + 16 + r * 8, 16, m)
                store(sums, 64 + r * 32 + c * 8, c * 64 + r * 8, 48, m)
            store(sums, 64 + r * 32 + 24, 16 + r * 8, 16, m)
    keep_induction(3)

    @pl.when(above)
    def _():
        halo_up().start()

    keep_induction(1)
    keep_induction(2)

    wait_spectra(4)
    for m in range(8):
        sums = over_mixed(4, m)
        for r in range(2):
            for c in (1, 2):
                store(sums, r * 16 + (c - 1) * 8, c * 64 + 16 + r * 8, 16, m)

    for half in range(2):
        lanes = pl.ds(half * 128, 128)
        adv[:, :, :, :, lanes] = out[half, 0:192, :].reshape(3, 4, 2, 8, 128).astype(BF16)
    pltpu.make_async_copy(efin, efin, e_recv.at[1]).wait()
    for q in range(2):
        for s in range(4):
            for half in range(2):
                energy[q, s:s + 1, half * 128:(half + 1) * 128] = efin[(q * 4 + s) * 2 + half]

    shells = [ind[:, s].astype(F32) for s in range(4)]
    grad[:, 1] = ((shells[2] - shells[0]) * 0.5).astype(BF16)
    grad[:, 2] = ((shells[3] - shells[1]) * 0.5).astype(BF16)

    @pl.when(below)
    def _():
        halo_down().wait_send()
        halo_up().wait_recv()

    grad[:, 0] = ((shells[1] - low[...].astype(F32)) * 0.5).astype(BF16)

    @pl.when(above)
    def _():
        halo_up().wait_send()
        halo_down().wait_recv()

    grad[:, 3] = ((high[...].astype(F32) - shells[2]) * 0.5).astype(BF16)

    others = pl.ds(0, (HARM - 1) * 8)
    for group in range(4):
        sent = mode_part(wire, group, others)
        pltpu.make_async_copy(sent, sent, mode_send.at[group]).wait()
    for group in range(5):
        sent = spec.at[group, others, :]
        pltpu.make_async_copy(sent, sent, spec_send.at[group]).wait()
    pltpu.make_async_copy(erecv.at[pl.ds(0, 31)], erecv.at[pl.ds(0, 31)], e_send.at[0]).wait()
    pltpu.make_async_copy(efin.at[pl.ds(0, 15)], efin.at[pl.ds(0, 15)], e_send.at[1]).wait()


def local(velocity, magnetic, vorticity, current):
    vmem = pl.BlockSpec(memory_space=pltpu.VMEM)
    block = velocity.shape
    return pl.pallas_call(
        kernel,
        out_shape=(
            jax.ShapeDtypeStruct(block, BF16),
            jax.ShapeDtypeStruct(block, BF16),
            jax.ShapeDtypeStruct((2, 4, L), F32),
        ),
        in_specs=[pl.BlockSpec(memory_space=pl.ANY)] * 4,
        out_specs=(vmem,) * 3,
        scratch_shapes=[
            pltpu.VMEM((4,) + block, BF16),
            pltpu.VMEM((2, L * 8, 128), F32),
            pltpu.VMEM((8, 192, L), BF16),
            pltpu.VMEM((2, 48 * 64, 128), F32),
            pltpu.VMEM((GROUP, 384, 512), BF16),
            pltpu.VMEM((3, 3, 256, 128), F32),
            pltpu.VMEM((3, 3, 256, 128), BF16),
            pltpu.VMEM((3, 3, 256, 128), BF16),
            pltpu.VMEM((2, 256, NPHI), BF16),
            pltpu.VMEM((256, 256), BF16),
            pltpu.VMEM((3, 128, 256), BF16),
            pltpu.VMEM((128, NPHI), F32),
            pltpu.VMEM((192, NPHI), F32),
            pltpu.VMEM((3, 256, NPHI), BF16),
            pltpu.VMEM((128, NPHI), BF16),
            pltpu.VMEM((5, 256, 128), BF16),
            pltpu.VMEM((5, 256, 128), BF16),
            pltpu.VMEM((5, 256, 128), F32),
            pltpu.VMEM((8, 128, L), F32),
            pltpu.VMEM((2, 384, 128), F32),
            pltpu.VMEM((3, 4, 2, 8, L), BF16),
            pltpu.VMEM((3, 2, 8, L), BF16),
            pltpu.VMEM((3, 2, 8, L), BF16),
            pltpu.VMEM((16, 1, 128), F32),
            pltpu.VMEM((HARM, 1, 128), F32),
            pltpu.VMEM((1, 1, 128), F32),
            pltpu.VMEM((16, 1, 128), F32),
            pltpu.SemaphoreType.DMA((4,)),
            pltpu.SemaphoreType.DMA((4,)),
            pltpu.SemaphoreType.DMA((4,)),
            pltpu.SemaphoreType.DMA((5,)),
            pltpu.SemaphoreType.DMA((5,)),
            pltpu.SemaphoreType.DMA((2,)),
            pltpu.SemaphoreType.DMA((2,)),
            pltpu.SemaphoreType.DMA((2,)),
            pltpu.SemaphoreType.DMA((2,)),
        ],
        compiler_params=pltpu.CompilerParams(collective_id=0, has_side_effects=True),
    )(velocity, magnetic, vorticity, current)


def solution(mesh):
    split = P(None, "rad", None, "harm", None)
    return jax.shard_map(
        local,
        mesh=mesh,
        in_specs=(split,) * 4,
        out_specs=(split, split, P(None, "rad", None)),
        check_vma=False,
    )
```

```python
import jax
import jax.numpy as jnp
from jax import lax
from jax.experimental import pallas as pl
from jax.experimental.pallas import tpu as pltpu
from jax.sharding import PartitionSpec as P

F32 = jnp.float32
BF16 = jnp.bfloat16
PI = 3.14159265358979
L = 256
HARM = 32
RAD = 16
NPHI = 768
GROUP = 8

PAIRS = ((0, 3), (1, 2))
EARLY = [(c, 0) for c in range(8)]
LATER = [(c, 0) for c in range(8, 12)] + [(c, 1) for c in range(12)]
SLOT_ROW = {}
for at, (c, pair) in enumerate(EARLY):
    for r in range(2):
        SLOT_ROW[c, pair, r] = r * 64 + at * 8
for at, (c, pair) in enumerate(LATER):
    for r in range(2):
        SLOT_ROW[c, pair, r] = 128 + r * 128 + at * 8
ROW_SLOT = {row: slot for slot, row in SLOT_ROW.items()}


def sin_poly(y):
    z = y * y
    s = -1.0 / 39916800.0
    for c in (1.0 / 362880.0, -1.0 / 5040.0, 1.0 / 120.0, -1.0 / 6.0, 1.0):
        s = s * z + c
    return y * s


def cos_768(q):
    return sin_poly((192.0 - jnp.minimum(q, 768.0 - q)) * (PI / 384.0))


def mod_768(v):
    return v - 768.0 * jnp.floor((v + 0.5) * (1.0 / 768.0))


def iota(shape, dim):
    return lax.broadcasted_iota(jnp.int32, shape, dim)


def fiota(shape, dim):
    return iota(shape, dim).astype(F32)


def parity_sign(order, rows=1):
    return 1.0 - 2.0 * ((iota((rows, L), 1) + order) & 1).astype(F32)


def dot_nt(a, b):
    return lax.dot_general(a, b, (((1,), (1,)), ((), ())), preferred_element_type=F32)


def dot_tn(a, b):
    return lax.dot_general(a, b, (((0,), (0,)), ((), ())), preferred_element_type=F32)


def legendre_steps(me, tab):
    order = (me * 8 + iota((8, 128), 0)).astype(F32)
    order_sq = order * order
    degree = fiota((8, L), 1)
    own = (me * 8 + iota((8, L), 0)).astype(F32)
    logs = 0.5 * jnp.log((2.0 * degree + 1.0) / jnp.maximum(2.0 * degree, 1.0))
    taken = jnp.where((degree >= 1.0) & (degree <= own), logs, 0.0)
    log_start = 0.5 * jnp.log(jnp.full((8, 1), 0.5, F32)) + jnp.sum(taken, axis=1, keepdims=True)
    cosine, sector, unscale = [], [], []
    for jt in range(2):
        odd = 2.0 * (fiota((8, 128), 1) + 128.0 * jt) + 1.0
        cosine.append(sin_poly((384.0 - odd) * (PI / 768.0)))
        sine = sin_poly(jnp.minimum(odd, 768.0 - odd) * (PI / 768.0))
        log_sector = log_start + order * jnp.log(sine)
        sector.append(jnp.exp(jnp.maximum(log_sector, -60.0)))
        unscale.append(jnp.exp(jnp.minimum(log_sector + 60.0, 0.0)))
    zero = jnp.zeros((8, 128), F32)
    per = 16

    def block(index, state):
        q0, p0, q1, p1, back = state
        for inner in range(per):
            deg_i = index * per + inner
            deg = deg_i.astype(F32)
            sq = deg * deg
            live = order < deg
            t = (4.0 * sq - 1.0) / jnp.where(live, sq - order_sq, 1.0)
            a = jnp.where(live, jnp.sqrt(t), 0.0)
            ab = a * back
            back = jnp.where(live, lax.rsqrt(t), 0.0)
            start = order == deg
            n0 = a * cosine[0] * q0 + (jnp.where(start, sector[0], 0.0) - ab * p0)
            n1 = a * cosine[1] * q1 + (jnp.where(start, sector[1], 0.0) - ab * p1)
            row = pl.ds(pl.multiple_of(deg_i * 8, 8), 8)
            tab[0, row, :] = n0 * unscale[0]
            tab[1, row, :] = n1 * unscale[1]
            q0, p0, q1, p1 = n0, q0, n1, q1
        return q0, p0, q1, p1, back

    lax.fori_loop(0, L // per, block, (zero, zero, zero, zero, zero))


def kernel(
    vel, mag, vor, cur,
    adv, grad, energy,
    fields,
    tab, qt, coef, rhs, synth, wire, modes, trig, turned, turned_early, grid, grid_early,
    prod, prod_early, spec, back, backf,
    acc, out, ind, low, high, esrc, erecv, ered, efin,
    field_sem, mode_send, mode_recv, spec_send, spec_recv, halo_send, halo_recv, e_send, e_recv,
):
    me = lax.axis_index("harm")
    my_rad = lax.axis_index("rad")
    above = my_rad < RAD - 1
    below = my_rad > 0

    def peer(i):
        return lax.rem(me + i, HARM)

    barrier = pltpu.get_barrier_semaphore()

    def greet(i, carry):
        pl.semaphore_signal(barrier, inc=1, device_id={"harm": peer(i)})
        return carry

    lax.fori_loop(1, HARM, greet, 0)

    @pl.when(above)
    def _():
        pl.semaphore_signal(barrier, inc=1, device_id={"rad": my_rad + 1})

    @pl.when(below)
    def _():
        pl.semaphore_signal(barrier, inc=1, device_id={"rad": my_rad - 1})

    arrivals = [
        pltpu.make_async_copy(ref, fields.at[a], field_sem.at[a])
        for a, ref in enumerate((vel, mag, vor, cur))
    ]
    for arrival in arrivals:
        arrival.start()

    @pl.when(jnp.logical_not(below))
    def _():
        low[...] = jnp.zeros(low.shape, BF16)

    @pl.when(jnp.logical_not(above))
    def _():
        high[...] = jnp.zeros(high.shape, BF16)

    legendre_steps(me, tab)

    for a, arrival in enumerate(arrivals):
        arrival.wait()
        for c in range(3):
            for r in range(2):
                for pair in range(2):
                    both = fields[a, c, PAIRS[pair][0], r], fields[a, c, PAIRS[pair][1], r]
                    both = jnp.concatenate([v.astype(F32) for v in both], axis=0)
                    at = ((r * 12 + a * 3 + c) * 2 + pair) * 64
                    for half in range(2):
                        part = both[:, half * 128:(half + 1) * 128]
                        for copy in range(4):
                            coef[half, at + copy * 16:at + copy * 16 + 16, :] = part

    slot_row = iota((8, 128), 0)

    def synthesis(m, slot):
        for jt, rows in ((0, 128), (1, 64)):
            table = tab[jt, pl.ds(m, L, stride=8), :]
            qt[m, jt * 128:jt * 128 + rows, :] = table.T[0:rows].astype(BF16)
        sign = parity_sign(m, 8)
        for half in range(2):
            sgn = jnp.where(slot_row >= 4, sign[:, half * 128:(half + 1) * 128], 1.0)
            keep = [jnp.where(((slot_row >> 1) & 1) == gn, sgn, 0.0) for gn in range(2)]
            for row in range(0, 384, 16):
                values = []
                for at in (row, row + 8):
                    c, pair, r = ROW_SLOT[at]
                    first = ((r * 12 + c) * 2 + pair) * 64
                    values.append(coef[half, pl.ds(first + m, 8, stride=8), :])
                for gn in range(2):
                    lane = gn * 256 + half * 128
                    rhs[slot, row:row + 16, lane:lane + 128] = jnp.concatenate(
                        [v * keep[gn] for v in values], axis=0
                    ).astype(BF16)
        lhs = jnp.concatenate([qt[m, 0:96, :], qt[m, 96:192, :]], axis=1)
        made = dot_nt(lhs, rhs[slot]) * (1.0 / L)
        for k in range(3):
            for lt in range(3):
                synth[k, lt, pl.ds(m, 32, stride=8), :] = made[
                    k * 32:(k + 1) * 32, lt * 128:(lt + 1) * 128
                ]

    def synthesis_group(group, carry):
        for inner in range(GROUP):
            synthesis(group * GROUP + inner, inner)
        return carry

    lax.fori_loop(0, 8 // GROUP, synthesis_group, 0)
    wire[...] = synth[...].astype(BF16)

    pl.semaphore_wait(barrier, HARM - 1 + above.astype(jnp.int32) + below.astype(jnp.int32))

    def rows_of(device):
        return pl.ds(pl.multiple_of(device * 8, 8), 8)

    def mode_part(ref, group, rows):
        if group == 0:
            return ref.at[:, 0, rows, :]
        return ref.at[group - 1, pl.ds(1, 2), rows, :]

    def send_modes(group):
        def one(i, carry):
            to = peer(i)
            pltpu.make_async_remote_copy(
                src_ref=mode_part(wire, group, rows_of(to)),
                dst_ref=mode_part(modes, group, rows_of(me)),
                send_sem=mode_send.at[group],
                recv_sem=mode_recv.at[group],
                device_id={"harm": to},
            ).start()
            return carry

        lax.fori_loop(1, HARM, one, 0)
        pltpu.make_async_copy(
            mode_part(wire, group, rows_of(me)),
            mode_part(modes, group, rows_of(me)),
            mode_recv.at[group],
        ).start()

    def wait_modes(group):
        landed = mode_part(modes, group, pl.ds(0, 256))
        pltpu.make_async_copy(landed, landed, mode_recv.at[group]).wait()

    for group in range(3):
        send_modes(group)

    order8 = me * 8 + iota((8, 128), 0)
    for half in range(2):
        degree = iota((8, 128), 1) + 128 * half
        weight = jnp.where(degree >= order8, 1.0 / (2.0 * degree.astype(F32) + 1.0), 0.0)
        weights = (
            weight * jnp.where(order8 == 0, 0.5, 1.0),
            weight * jnp.where(order8 == 0, 0.0, 1.0),
        )
        for q in range(2):
            for s in range(4):
                pair = 0 if s in PAIRS[0] else 1
                total = jnp.zeros((8, 128), F32)
                for c in range(3):
                    for r in range(2):
                        at = ((r * 12 + q * 3 + c) * 2 + pair) * 64 + PAIRS[pair].index(s) * 8
                        value = coef[half, at:at + 8, :]
                        total += value * value * weights[r]
                esrc[(q * 4 + s) * 2 + half] = jnp.sum(total, axis=0, keepdims=True)

    def send_energy(i, carry):
        to = peer(i)
        pltpu.make_async_remote_copy(
            src_ref=esrc.at[lax.rem(to, 16)],
            dst_ref=erecv.at[me],
            send_sem=e_send.at[0],
            recv_sem=e_recv.at[0],
            device_id={"harm": to},
        ).start()
        return carry

    lax.fori_loop(1, HARM, send_energy, 0)
    pltpu.make_async_copy(esrc.at[lax.rem(me, 16)], erecv.at[me], e_recv.at[0]).start()

    def trig_rows(b, carry):
        angle = mod_768((b * 8 + iota((8, NPHI), 0)).astype(F32) * fiota((8, NPHI), 1))
        rows = pl.ds(pl.multiple_of(b * 8, 8), 8)
        trig[0, rows, :] = cos_768(angle).astype(BF16)
        trig[1, rows, :] = cos_768(jnp.where(angle >= 192.0, angle - 192.0, angle + 576.0)).astype(BF16)
        return carry

    lax.fori_loop(0, 32, trig_rows, 0)

    lane = iota((1, 128), 1)
    factors = []
    for k in range(3):
        row = ((lane >> 1) & 1) * 96 + k * 32 + me
        wave = fiota((192, 128), 0) + 1.0
        odd = (2 * row + 1).astype(F32)
        series = cos_768(mod_768(wave * odd)) / (4.0 * wave * wave - 1.0)
        weight = (2.0 / 384.0) * (1.0 - 2.0 * jnp.sum(series, axis=0, keepdims=True))
        factors.append(weight * (256.0 / 768.0))
    mixed = jnp.where(lane < 32, factors[0], jnp.where(lane < 64, factors[1], factors[2]))
    mode_weight = jnp.where(iota((256, 1), 0) == 0, 1.0, 2.0)
    prod[:, 128:256, :] = jnp.zeros((3, 128, NPHI), BF16)
    prod_early[96:128, :] = jnp.zeros((32, NPHI), BF16)

    def cross(x, y, i):
        n, o = (i + 1) % 3, (i + 2) % 3
        return x[n] * y[o] - x[o] * y[n]

    def rounded_pair(first, second):
        return jnp.concatenate([first, second], axis=0).astype(BF16)

    def send_spectra(group):
        def one(i, carry):
            to = peer(i)
            pltpu.make_async_remote_copy(
                src_ref=spec.at[group, rows_of(to), :],
                dst_ref=back.at[group, rows_of(me), :],
                send_sem=spec_send.at[group],
                recv_sem=spec_recv.at[group],
                device_id={"harm": to},
            ).start()
            return carry

        lax.fori_loop(1, HARM, one, 0)
        pltpu.make_async_copy(
            spec.at[group, rows_of(me), :], back.at[group, rows_of(me), :], spec_recv.at[group]
        ).start()

    def wait_spectra(group):
        pltpu.make_async_copy(back.at[group], back.at[group], spec_recv.at[group]).wait()
        backf[group] = back[group].astype(F32)

    wait_modes(0)
    for k in range(3):
        turned_early[k] = modes[k, 0].T
    grid_early[...] = sum(
        jnp.dot(
            jnp.concatenate([turned_early[k, r * 64:(r + 1) * 64] for k in range(3)], axis=0),
            trig[r], preferred_element_type=F32,
        )
        for r in range(2)
    )
    even_row = (iota((8, 128), 0) & 1) == 0
    for k in range(3):
        for pt in range(6):
            cols = slice(pt * 128, (pt + 1) * 128)
            g = [grid_early[k * 64 + c * 8:k * 64 + c * 8 + 8, cols] for c in range(6)]
            x, y, z = (cross(g[0:3], g[3:6], i) for i in range(3))
            lower = jnp.where(even_row, x, pltpu.roll(y, 1, 0))
            upper = jnp.where(even_row, pltpu.roll(x, 7, 0), y).astype(BF16)
            pair = rounded_pair(lower, z)
            for r in range(2):
                prod_early[k * 32 + r * 16:k * 32 + r * 16 + 16, cols] = pair
                prod[k, r * 32:r * 32 + 8, cols] = upper
    early_c, early_s = (dot_nt(trig[r], prod_early[...]) for r in range(2))
    spec[0] = (
        jnp.where(((lane >> 4) & 1) == 0, early_c, early_s) * (mode_weight * mixed)
    ).astype(BF16)
    send_spectra(0)
    send_modes(3)

    def later(k):
        for lt in range(2):
            turned[lt * 128:(lt + 1) * 128, :] = modes[k, 1 + lt].T
        grid[...] = sum(
            jnp.dot(turned[r * 128:(r + 1) * 128], trig[r], preferred_element_type=F32)
            for r in range(2)
        )
        for pt in range(6):
            cols = slice(pt * 128, (pt + 1) * 128)

            def value(c, pair):
                if pair == 0 and c < 8:
                    return grid_early[k * 64 + c * 8:k * 64 + c * 8 + 8, cols]
                at = (c - 8) * 8 if pair == 0 else 32 + c * 8
                return grid[at:at + 8, cols]

            u, b, w, j = ([value(v * 3 + i, 1) for i in range(3)] for v in range(4))
            inner = [cross(u, w, i) + cross(j, b, i) for i in range(3)]
            curl = [cross(u, b, i) for i in range(3)]
            u, b, w, j = ([value(v * 3 + i, 0) for i in range(3)] for v in range(4))
            ends = [cross(u, w, i) + cross(j, b, i) for i in range(3)]
            for r in range(2):
                prod[k, r * 32 + 8:r * 32 + 16, cols] = curl[0].astype(BF16)
                prod[k, r * 32 + 16:r * 32 + 32, cols] = rounded_pair(curl[1], curl[2])
                prod[k, 64 + r * 32:64 + r * 32 + 16, cols] = rounded_pair(ends[0], ends[1])
                prod[k, 80 + r * 32:80 + r * 32 + 16, cols] = rounded_pair(ends[2], inner[0])
                at = 128 + 32 * k + 16 * r
                prod[k, at:at + 16, cols] = rounded_pair(inner[1], inner[2])
        cosine, sine = (dot_nt(trig[r], prod[k]) for r in range(2))
        scale = mode_weight * factors[k]
        lead = jnp.where(((lane >> 5) & 1) == 0, cosine[:, 0:128], sine[:, 0:128]) * scale
        trail = jnp.where(((lane >> 4) & 1) == 0, cosine[:, 128:256], sine[:, 128:256]) * scale
        spec[1 + k] = lead.astype(BF16)
        return trail

    wait_modes(1)
    trail = later(0)
    send_spectra(1)

    col = iota((32, 128), 1)
    col_gn = (col >> 1) & 1

    def column(tile, m):
        return backf[tile, pl.ds(m, 32, stride=8), :]

    def table(m, ks):
        return jnp.concatenate(
            [qt[m, gn * 96 + ks[0] * 32:gn * 96 + ks[-1] * 32 + 32, :] for gn in range(2)], axis=0
        )

    def over_rows(values, m, ks):
        kept = jnp.concatenate(
            [jnp.where(col_gn == gn, part, 0.0) for gn in range(2) for part in values], axis=0
        ).astype(BF16)
        return dot_tn(kept, table(m, ks))

    def over_mixed(tile, m):
        values = column(tile, m)
        sums = over_rows(
            [jnp.where((col >> 5) == k, values, 0.0) for k in range(3)], m, (0, 1, 2)
        )
        return sums[0:32] + sums[32:64] + sums[64:96]

    lower_half = iota((8, L), 0) < 4

    def store(sums, at, row, stride, m):
        v = sums[at:at + 8] * jnp.where(lower_half, 1.0, parity_sign(m, 8))
        v = v + pltpu.roll(v, 4, 0)
        v = v + pltpu.roll(v, 6, 0)
        for half in range(2):
            out[half, pl.ds(row + m, 2, stride=stride), :] = v[0:2, half * 128:(half + 1) * 128]

    def keep_induction(s):
        for c in range(3):
            for half in range(2):
                rows = 192 + c * 64 + s * 16
                lanes = pl.ds(half * 128, 128)
                ind[c, s, :, :, lanes] = out[half, rows:rows + 16, :].reshape(2, 8, 128).astype(BF16)

    def halo_down():
        return pltpu.make_async_remote_copy(
            src_ref=ind.at[:, 0], dst_ref=high, send_sem=halo_send.at[1], recv_sem=halo_recv.at[1],
            device_id={"rad": my_rad - 1},
        )

    def halo_up():
        return pltpu.make_async_remote_copy(
            src_ref=ind.at[:, 3], dst_ref=low, send_sem=halo_send.at[0], recv_sem=halo_recv.at[0],
            device_id={"rad": my_rad + 1},
        )

    wait_spectra(0)
    for m in range(8):
        sums = over_mixed(0, m)
        for r in range(2):
            store(sums, r * 16, 192 + r * 8, 64, m)
            store(sums, r * 16 + 8, 192 + 128 + r * 8, 48, m)
    keep_induction(0)

    @pl.when(below)
    def _():
        halo_down().start()

    wait_modes(2)
    trail = jnp.where((lane >> 5) == 1, later(1), trail)
    send_spectra(2)

    pltpu.make_async_copy(erecv, erecv, e_recv.at[0]).wait()
    ered[...] = jnp.sum(erecv[...], axis=0, keepdims=True)
    mine = lax.rem(me, 16)

    def send_row(i, carry):
        pltpu.make_async_remote_copy(
            src_ref=ered.at[0],
            dst_ref=efin.at[mine],
            send_sem=e_send.at[1],
            recv_sem=e_recv.at[1],
            device_id={"harm": me - mine + lax.rem(mine + i, 16)},
        ).start()
        return carry

    lax.fori_loop(1, 16, send_row, 0)
    pltpu.make_async_copy(ered.at[0], efin.at[mine], e_recv.at[1]).start()

    wait_modes(3)
    trail = jnp.where((lane >> 5) == 2, later(2), trail)
    send_spectra(3)
    spec[4] = trail.astype(BF16)
    send_spectra(4)

    wait_spectra(1)
    wait_spectra(2)
    for m in range(8):
        acc[m] = over_rows([column(1, m), column(2, m)], m, (0, 1))
    wait_spectra(3)
    for m in range(8):
        sums = acc[m] + over_rows([column(3, m)], m, (2,))
        for r in range(2):
            store(sums, r * 32, 192 + 48 + r * 8, 64, m)
            for c in range(3):
                store(sums, r * 32 + 8 + c * 8, 192 + c * 64 + 16 + r * 8, 16, m)
                store(sums, 64 + r * 32 + c * 8, c * 64 + r * 8, 48, m)
            store(sums, 64 + r * 32 + 24, 16 + r * 8, 16, m)
    keep_induction(3)

    @pl.when(above)
    def _():
        halo_up().start()

    keep_induction(1)
    keep_induction(2)

    wait_spectra(4)
    for m in range(8):
        sums = over_mixed(4, m)
        for r in range(2):
            for c in (1, 2):
                store(sums, r * 16 + (c - 1) * 8, c * 64 + 16 + r * 8, 16, m)

    for half in range(2):
        lanes = pl.ds(half * 128, 128)
        adv[:, :, :, :, lanes] = out[half, 0:192, :].reshape(3, 4, 2, 8, 128).astype(BF16)
    pltpu.make_async_copy(efin, efin, e_recv.at[1]).wait()
    for q in range(2):
        for s in range(4):
            for half in range(2):
                energy[q, s:s + 1, half * 128:(half + 1) * 128] = efin[(q * 4 + s) * 2 + half]

    shells = [ind[:, s].astype(F32) for s in range(4)]
    grad[:, 1] = ((shells[2] - shells[0]) * 0.5).astype(BF16)
    grad[:, 2] = ((shells[3] - shells[1]) * 0.5).astype(BF16)

    @pl.when(below)
    def _():
        halo_down().wait_send()
        halo_up().wait_recv()

    grad[:, 0] = ((shells[1] - low[...].astype(F32)) * 0.5).astype(BF16)

    @pl.when(above)
    def _():
        halo_up().wait_send()
        halo_down().wait_recv()

    grad[:, 3] = ((high[...].astype(F32) - shells[2]) * 0.5).astype(BF16)

    others = pl.ds(0, (HARM - 1) * 8)
    for group in range(4):
        sent = mode_part(wire, group, others)
        pltpu.make_async_copy(sent, sent, mode_send.at[group]).wait()
    for group in range(5):
        sent = spec.at[group, others, :]
        pltpu.make_async_copy(sent, sent, spec_send.at[group]).wait()
    pltpu.make_async_copy(erecv.at[pl.ds(0, 31)], erecv.at[pl.ds(0, 31)], e_send.at[0]).wait()
    pltpu.make_async_copy(efin.at[pl.ds(0, 15)], efin.at[pl.ds(0, 15)], e_send.at[1]).wait()


def hand_out(adv, grad, energy, adv_out, grad_out, energy_out, sem):
    copies = [
        pltpu.make_async_copy(source, target, sem.at[i])
        for i, (source, target) in enumerate(
            ((adv, adv_out), (grad, grad_out), (energy, energy_out))
        )
    ]
    for copy in copies:
        copy.start()
    for copy in copies:
        copy.wait()


def local(velocity, magnetic, vorticity, current):
    vmem = pl.BlockSpec(memory_space=pltpu.VMEM)
    block = velocity.shape
    made = pl.pallas_call(
        kernel,
        out_shape=(
            jax.ShapeDtypeStruct(block, BF16),
            jax.ShapeDtypeStruct(block, BF16),
            jax.ShapeDtypeStruct((2, 4, L), F32),
        ),
        in_specs=[pl.BlockSpec(memory_space=pltpu.HBM)] * 4,
        out_specs=(vmem,) * 3,
        scratch_shapes=[
            pltpu.VMEM((4,) + block, BF16),
            pltpu.VMEM((2, L * 8, 128), F32),
            pltpu.VMEM((8, 192, L), BF16),
            pltpu.VMEM((2, 48 * 64, 128), F32),
            pltpu.VMEM((GROUP, 384, 512), BF16),
            pltpu.VMEM((3, 3, 256, 128), F32),
            pltpu.VMEM((3, 3, 256, 128), BF16),
            pltpu.VMEM((3, 3, 256, 128), BF16),
            pltpu.VMEM((2, 256, NPHI), BF16),
            pltpu.VMEM((256, 256), BF16),
            pltpu.VMEM((3, 128, 256), BF16),
            pltpu.VMEM((128, NPHI), F32),
            pltpu.VMEM((192, NPHI), F32),
            pltpu.VMEM((3, 256, NPHI), BF16),
            pltpu.VMEM((128, NPHI), BF16),
            pltpu.VMEM((5, 256, 128), BF16),
            pltpu.VMEM((5, 256, 128), BF16),
            pltpu.VMEM((5, 256, 128), F32),
            pltpu.VMEM((8, 128, L), F32),
            pltpu.VMEM((2, 384, 128), F32),
            pltpu.VMEM((3, 4, 2, 8, L), BF16),
            pltpu.VMEM((3, 2, 8, L), BF16),
            pltpu.VMEM((3, 2, 8, L), BF16),
            pltpu.VMEM((16, 1, 128), F32),
            pltpu.VMEM((HARM, 1, 128), F32),
            pltpu.VMEM((1, 1, 128), F32),
            pltpu.VMEM((16, 1, 128), F32),
            pltpu.SemaphoreType.DMA((4,)),
            pltpu.SemaphoreType.DMA((4,)),
            pltpu.SemaphoreType.DMA((4,)),
            pltpu.SemaphoreType.DMA((5,)),
            pltpu.SemaphoreType.DMA((5,)),
            pltpu.SemaphoreType.DMA((2,)),
            pltpu.SemaphoreType.DMA((2,)),
            pltpu.SemaphoreType.DMA((2,)),
            pltpu.SemaphoreType.DMA((2,)),
        ],
        compiler_params=pltpu.CompilerParams(
            collective_id=0, has_side_effects=True, vmem_limit_bytes=40 * 1024 * 1024
        ),
    )(*(pltpu.with_memory_space_constraint(v, pltpu.HBM) for v in (velocity, magnetic, vorticity, current)))
    return pl.pallas_call(
        hand_out,
        out_shape=tuple(jax.ShapeDtypeStruct(v.shape, v.dtype) for v in made),
        in_specs=[pl.BlockSpec(memory_space=pl.ANY)] * 3,
        out_specs=(pl.BlockSpec(memory_space=pltpu.HBM),) * 3,
        scratch_shapes=[pltpu.SemaphoreType.DMA((3,))],
        compiler_params=pltpu.CompilerParams(vmem_limit_bytes=1024 * 1024),
    )(*made)


def solution(mesh):
    split = P(None, "rad", None, "harm", None)
    return jax.shard_map(
        local,
        mesh=mesh,
        in_specs=(split,) * 4,
        out_specs=(split, split, P(None, "rad", None)),
        check_vma=False,
    )
```

```python
import jax
import jax.numpy as jnp
from jax import lax
from jax.experimental import pallas as pl
from jax.experimental.pallas import tpu as pltpu
from jax.sharding import PartitionSpec as P

F32 = jnp.float32
BF16 = jnp.bfloat16
PI = 3.14159265358979
L = 256
HARM = 32
RAD = 16
NPHI = 768

PAIRS = ((0, 3), (1, 2))
EARLY = [(c, 0) for c in range(8)]
LATER = [(c, 0) for c in range(8, 12)] + [(c, 1) for c in range(12)]
SLOT_ROW = {}
for at, (c, pair) in enumerate(EARLY):
    for r in range(2):
        SLOT_ROW[c, pair, r] = r * 64 + at * 8
for at, (c, pair) in enumerate(LATER):
    for r in range(2):
        SLOT_ROW[c, pair, r] = 128 + r * 128 + at * 8
ROW_SLOT = {row: slot for slot, row in SLOT_ROW.items()}


def sin_poly(y):
    z = y * y
    s = -1.0 / 39916800.0
    for c in (1.0 / 362880.0, -1.0 / 5040.0, 1.0 / 120.0, -1.0 / 6.0, 1.0):
        s = s * z + c
    return y * s


def cos_768(q):
    return sin_poly((192.0 - jnp.minimum(q, 768.0 - q)) * (PI / 384.0))


def mod_768(v):
    return v - 768.0 * jnp.floor((v + 0.5) * (1.0 / 768.0))


def iota(shape, dim):
    return lax.broadcasted_iota(jnp.int32, shape, dim)


def fiota(shape, dim):
    return iota(shape, dim).astype(F32)


def parity_sign(order, rows=1):
    return 1.0 - 2.0 * ((iota((rows, L), 1) + order) & 1).astype(F32)


def dot_nt(a, b):
    return lax.dot_general(a, b, (((1,), (1,)), ((), ())), preferred_element_type=F32)


def dot_tn(a, b):
    return lax.dot_general(a, b, (((0,), (0,)), ((), ())), preferred_element_type=F32)


def legendre_steps(me, tab):
    order = (me * 8 + iota((8, 128), 0)).astype(F32)
    order_sq = order * order
    degree = fiota((8, L), 1)
    own = (me * 8 + iota((8, L), 0)).astype(F32)
    logs = 0.5 * jnp.log((2.0 * degree + 1.0) / jnp.maximum(2.0 * degree, 1.0))
    taken = jnp.where((degree >= 1.0) & (degree <= own), logs, 0.0)
    log_start = 0.5 * jnp.log(jnp.full((8, 1), 0.5, F32)) + jnp.sum(taken, axis=1, keepdims=True)
    cosine, sector, unscale = [], [], []
    for jt in range(2):
        odd = 2.0 * (fiota((8, 128), 1) + 128.0 * jt) + 1.0
        cosine.append(sin_poly((384.0 - odd) * (PI / 768.0)))
        sine = sin_poly(jnp.minimum(odd, 768.0 - odd) * (PI / 768.0))
        log_sector = log_start + order * jnp.log(sine)
        sector.append(jnp.exp(jnp.maximum(log_sector, -60.0)))
        unscale.append(jnp.exp(jnp.minimum(log_sector + 60.0, 0.0)))
    zero = jnp.zeros((8, 128), F32)
    per = 16

    def block(index, state):
        q0, p0, q1, p1, back = state
        for inner in range(per):
            deg_i = index * per + inner
            deg = deg_i.astype(F32)
            sq = deg * deg
            live = order < deg
            t = (4.0 * sq - 1.0) / jnp.where(live, sq - order_sq, 1.0)
            a = jnp.where(live, jnp.sqrt(t), 0.0)
            ab = a * back
            back = jnp.where(live, lax.rsqrt(t), 0.0)
            start = order == deg
            n0 = a * cosine[0] * q0 + (jnp.where(start, sector[0], 0.0) - ab * p0)
            n1 = a * cosine[1] * q1 + (jnp.where(start, sector[1], 0.0) - ab * p1)
            row = pl.ds(pl.multiple_of(deg_i * 8, 8), 8)
            tab[0, row, :] = n0 * unscale[0]
            tab[1, row, :] = n1 * unscale[1]
            q0, p0, q1, p1 = n0, q0, n1, q1
        return q0, p0, q1, p1, back

    lax.fori_loop(0, L // per, block, (zero, zero, zero, zero, zero))


def kernel(
    vel, mag, vor, cur,
    adv, grad, energy,
    fields,
    tab, qt, coef, rhs, synth, wire, modes, trig, turned, turned_early, grid, grid_early,
    prod, prod_early, spec, back, backf,
    acc, out, ind, low, high, esrc, erecv, ered, efin,
    field_sem, mode_send, mode_recv, spec_send, spec_recv, halo_send, halo_recv, e_send, e_recv,
):
    me = lax.axis_index("harm")
    my_rad = lax.axis_index("rad")
    above = my_rad < RAD - 1
    below = my_rad > 0

    def peer(i):
        return lax.rem(me + i, HARM)

    barrier = pltpu.get_barrier_semaphore()

    def greet(i, carry):
        pl.semaphore_signal(barrier, inc=1, device_id={"harm": peer(i)})
        return carry

    lax.fori_loop(1, HARM, greet, 0)

    @pl.when(above)
    def _():
        pl.semaphore_signal(barrier, inc=1, device_id={"rad": my_rad + 1})

    arrivals = [
        pltpu.make_async_copy(ref, fields.at[a], field_sem.at[a])
        for a, ref in enumerate((vel, mag, vor, cur))
    ]
    for arrival in arrivals:
        arrival.start()

    @pl.when(jnp.logical_not(below))
    def _():
        low[...] = jnp.zeros(low.shape, BF16)

    @pl.when(jnp.logical_not(above))
    def _():
        high[...] = jnp.zeros(high.shape, BF16)

    legendre_steps(me, tab)

    def spread(c, pair):
        for r in range(2):
            both = [fields[c // 3, c % 3, shell, r].astype(F32) for shell in PAIRS[pair]]
            both = jnp.concatenate(both, axis=0)
            at = ((r * 12 + c) * 2 + pair) * 64
            for half in range(2):
                part = both[:, half * 128:(half + 1) * 128]
                for copy in range(4):
                    coef[half, at + copy * 16:at + copy * 16 + 16, :] = part

    for arrival in arrivals:
        arrival.wait()
    for c, pair in EARLY:
        spread(c, pair)

    slot_row = iota((8, 128), 0)

    def synthesis(m, tiles):
        first_row, last_row = tiles[0] * 128, tiles[-1] * 128 + 128
        sign = parity_sign(m, 8)
        for half in range(2):
            sgn = jnp.where(slot_row >= 4, sign[:, half * 128:(half + 1) * 128], 1.0)
            keep = [jnp.where(((slot_row >> 1) & 1) == gn, sgn, 0.0) for gn in range(2)]
            for row in range(first_row, last_row, 16):
                values = []
                for at in (row, row + 8):
                    c, pair, r = ROW_SLOT[at]
                    first = ((r * 12 + c) * 2 + pair) * 64
                    values.append(coef[half, pl.ds(first + m, 8, stride=8), :])
                for gn in range(2):
                    lane = gn * 256 + half * 128
                    rhs[m, row:row + 16, lane:lane + 128] = jnp.concatenate(
                        [v * keep[gn] for v in values], axis=0
                    ).astype(BF16)
        lhs = jnp.concatenate([qt[m, 0:96, :], qt[m, 96:192, :]], axis=1)
        made = dot_nt(lhs, rhs[m, first_row:last_row]) * (1.0 / L)
        for k in range(3):
            for lt in tiles:
                lane = lt * 128 - first_row
                synth[k, lt, pl.ds(m, 32, stride=8), :] = made[
                    k * 32:(k + 1) * 32, lane:lane + 128
                ]

    for m in range(8):
        for jt, rows in ((0, 128), (1, 64)):
            table_of = tab[jt, pl.ds(m, L, stride=8), :]
            qt[m, jt * 128:jt * 128 + rows, :] = table_of.T[0:rows].astype(BF16)
        synthesis(m, (0,))
    wire[:, 0] = synth[:, 0].astype(BF16)

    pl.semaphore_wait(barrier, HARM - 1 + below.astype(jnp.int32))

    def rows_of(device):
        return pl.ds(pl.multiple_of(device * 8, 8), 8)

    def mode_part(ref, group, rows):
        if group == 0:
            return ref.at[:, 0, rows, :]
        return ref.at[group - 1, pl.ds(1, 2), rows, :]

    def send_modes(group):
        def one(i, carry):
            to = peer(i)
            pltpu.make_async_remote_copy(
                src_ref=mode_part(wire, group, rows_of(to)),
                dst_ref=mode_part(modes, group, rows_of(me)),
                send_sem=mode_send.at[group],
                recv_sem=mode_recv.at[group],
                device_id={"harm": to},
            ).start()
            return carry

        lax.fori_loop(1, HARM, one, 0)
        pltpu.make_async_copy(
            mode_part(wire, group, rows_of(me)),
            mode_part(modes, group, rows_of(me)),
            mode_recv.at[group],
        ).start()

    def wait_modes(group):
        landed = mode_part(modes, group, pl.ds(0, 256))
        pltpu.make_async_copy(landed, landed, mode_recv.at[group]).wait()

    send_modes(0)

    for c, pair in LATER:
        spread(c, pair)
    for m in range(8):
        synthesis(m, (1, 2))
    wire[:, 1:3] = synth[:, 1:3].astype(BF16)
    send_modes(1)
    send_modes(2)

    order8 = me * 8 + iota((8, 128), 0)
    for half in range(2):
        degree = iota((8, 128), 1) + 128 * half
        weight = jnp.where(degree >= order8, 1.0 / (2.0 * degree.astype(F32) + 1.0), 0.0)
        weights = (
            weight * jnp.where(order8 == 0, 0.5, 1.0),
            weight * jnp.where(order8 == 0, 0.0, 1.0),
        )
        for q in range(2):
            for s in range(4):
                pair = 0 if s in PAIRS[0] else 1
                total = jnp.zeros((8, 128), F32)
                for c in range(3):
                    for r in range(2):
                        at = ((r * 12 + q * 3 + c) * 2 + pair) * 64 + PAIRS[pair].index(s) * 8
                        value = coef[half, at:at + 8, :]
                        total += value * value * weights[r]
                esrc[(q * 4 + s) * 2 + half] = jnp.sum(total, axis=0, keepdims=True)

    def send_energy(i, carry):
        to = peer(i)
        pltpu.make_async_remote_copy(
            src_ref=esrc.at[lax.rem(to, 16)],
            dst_ref=erecv.at[me],
            send_sem=e_send.at[0],
            recv_sem=e_recv.at[0],
            device_id={"harm": to},
        ).start()
        return carry

    lax.fori_loop(1, HARM, send_energy, 0)
    pltpu.make_async_copy(esrc.at[lax.rem(me, 16)], erecv.at[me], e_recv.at[0]).start()

    def trig_rows(b, carry):
        angle = mod_768((b * 8 + iota((8, NPHI), 0)).astype(F32) * fiota((8, NPHI), 1))
        rows = pl.ds(pl.multiple_of(b * 8, 8), 8)
        trig[0, rows, :] = cos_768(angle).astype(BF16)
        trig[1, rows, :] = cos_768(jnp.where(angle >= 192.0, angle - 192.0, angle + 576.0)).astype(BF16)
        return carry

    lax.fori_loop(0, 32, trig_rows, 0)

    lane = iota((1, 128), 1)
    factors = []
    for k in range(3):
        row = ((lane >> 1) & 1) * 96 + k * 32 + me
        wave = fiota((192, 128), 0) + 1.0
        odd = (2 * row + 1).astype(F32)
        series = cos_768(mod_768(wave * odd)) / (4.0 * wave * wave - 1.0)
        weight = (2.0 / 384.0) * (1.0 - 2.0 * jnp.sum(series, axis=0, keepdims=True))
        factors.append(weight * (256.0 / 768.0))
    mixed = jnp.where(lane < 32, factors[0], jnp.where(lane < 64, factors[1], factors[2]))
    mode_weight = jnp.where(iota((256, 1), 0) == 0, 1.0, 2.0)
    prod[:, 128:256, :] = jnp.zeros((3, 128, NPHI), BF16)
    prod_early[96:128, :] = jnp.zeros((32, NPHI), BF16)

    def cross(x, y, i):
        n, o = (i + 1) % 3, (i + 2) % 3
        return x[n] * y[o] - x[o] * y[n]

    def rounded_pair(first, second):
        return jnp.concatenate([first, second], axis=0).astype(BF16)

    def send_spectra(group):
        def one(i, carry):
            to = peer(i)
            pltpu.make_async_remote_copy(
                src_ref=spec.at[group, rows_of(to), :],
                dst_ref=back.at[group, rows_of(me), :],
                send_sem=spec_send.at[group],
                recv_sem=spec_recv.at[group],
                device_id={"harm": to},
            ).start()
            return carry

        lax.fori_loop(1, HARM, one, 0)
        pltpu.make_async_copy(
            spec.at[group, rows_of(me), :], back.at[group, rows_of(me), :], spec_recv.at[group]
        ).start()

    def wait_spectra(group):
        pltpu.make_async_copy(back.at[group], back.at[group], spec_recv.at[group]).wait()
        backf[group] = back[group].astype(F32)

    wait_modes(0)
    for k in range(3):
        turned_early[k] = modes[k, 0].T
    grid_early[...] = sum(
        jnp.dot(
            jnp.concatenate([turned_early[k, r * 64:(r + 1) * 64] for k in range(3)], axis=0),
            trig[r], preferred_element_type=F32,
        )
        for r in range(2)
    )
    even_row = (iota((8, 128), 0) & 1) == 0
    for k in range(3):
        for pt in range(6):
            cols = slice(pt * 128, (pt + 1) * 128)
            g = [grid_early[k * 64 + c * 8:k * 64 + c * 8 + 8, cols] for c in range(6)]
            x, y, z = (cross(g[0:3], g[3:6], i) for i in range(3))
            lower = jnp.where(even_row, x, pltpu.roll(y, 1, 0))
            upper = jnp.where(even_row, pltpu.roll(x, 7, 0), y).astype(BF16)
            pair = rounded_pair(lower, z)
            for r in range(2):
                prod_early[k * 32 + r * 16:k * 32 + r * 16 + 16, cols] = pair
                prod[k, r * 32:r * 32 + 8, cols] = upper
    early_c, early_s = (dot_nt(trig[r], prod_early[...]) for r in range(2))
    spec[0] = (
        jnp.where(((lane >> 4) & 1) == 0, early_c, early_s) * (mode_weight * mixed)
    ).astype(BF16)
    send_spectra(0)
    send_modes(3)

    def later(k):
        for lt in range(2):
            turned[lt * 128:(lt + 1) * 128, :] = modes[k, 1 + lt].T
        grid[...] = sum(
            jnp.dot(turned[r * 128:(r + 1) * 128], trig[r], preferred_element_type=F32)
            for r in range(2)
        )
        for pt in range(6):
            cols = slice(pt * 128, (pt + 1) * 128)

            def value(c, pair):
                if pair == 0 and c < 8:
                    return grid_early[k * 64 + c * 8:k * 64 + c * 8 + 8, cols]
                at = (c - 8) * 8 if pair == 0 else 32 + c * 8
                return grid[at:at + 8, cols]

            u, b, w, j = ([value(v * 3 + i, 1) for i in range(3)] for v in range(4))
            inner = [cross(u, w, i) + cross(j, b, i) for i in range(3)]
            curl = [cross(u, b, i) for i in range(3)]
            u, b, w, j = ([value(v * 3 + i, 0) for i in range(3)] for v in range(4))
            ends = [cross(u, w, i) + cross(j, b, i) for i in range(3)]
            for r in range(2):
                prod[k, r * 32 + 8:r * 32 + 16, cols] = curl[0].astype(BF16)
                prod[k, r * 32 + 16:r * 32 + 32, cols] = rounded_pair(curl[1], curl[2])
                prod[k, 64 + r * 32:64 + r * 32 + 16, cols] = rounded_pair(ends[0], ends[1])
                prod[k, 80 + r * 32:80 + r * 32 + 16, cols] = rounded_pair(ends[2], inner[0])
                at = 128 + 32 * k + 16 * r
                prod[k, at:at + 16, cols] = rounded_pair(inner[1], inner[2])
        cosine, sine = (dot_nt(trig[r], prod[k]) for r in range(2))
        scale = mode_weight * factors[k]
        lead = jnp.where(((lane >> 5) & 1) == 0, cosine[:, 0:128], sine[:, 0:128]) * scale
        trail = jnp.where(((lane >> 4) & 1) == 0, cosine[:, 128:256], sine[:, 128:256]) * scale
        spec[1 + k] = lead.astype(BF16)
        return trail

    wait_modes(1)
    trail = later(0)
    send_spectra(1)

    col = iota((32, 128), 1)
    col_gn = (col >> 1) & 1

    def column(tile, m):
        return backf[tile, pl.ds(m, 32, stride=8), :]

    def table(m, ks):
        return jnp.concatenate(
            [qt[m, gn * 96 + ks[0] * 32:gn * 96 + ks[-1] * 32 + 32, :] for gn in range(2)], axis=0
        )

    def over_rows(values, m, ks):
        kept = jnp.concatenate(
            [jnp.where(col_gn == gn, part, 0.0) for gn in range(2) for part in values], axis=0
        ).astype(BF16)
        return dot_tn(kept, table(m, ks))

    def over_mixed(tile, m):
        values = column(tile, m)
        sums = over_rows(
            [jnp.where((col >> 5) == k, values, 0.0) for k in range(3)], m, (0, 1, 2)
        )
        return sums[0:32] + sums[32:64] + sums[64:96]

    lower_half = iota((8, L), 0) < 4

    def store(sums, at, row, stride, m):
        v = sums[at:at + 8] * jnp.where(lower_half, 1.0, parity_sign(m, 8))
        v = v + pltpu.roll(v, 4, 0)
        v = v + pltpu.roll(v, 6, 0)
        for half in range(2):
            out[half, pl.ds(row + m, 2, stride=stride), :] = v[0:2, half * 128:(half + 1) * 128]

    def keep_induction(s):
        for c in range(3):
            for half in range(2):
                rows = 192 + c * 64 + s * 16
                lanes = pl.ds(half * 128, 128)
                ind[c, s, :, :, lanes] = out[half, rows:rows + 16, :].reshape(2, 8, 128).astype(BF16)

    def halo_down():
        return pltpu.make_async_remote_copy(
            src_ref=ind.at[:, 0], dst_ref=high, send_sem=halo_send.at[1], recv_sem=halo_recv.at[1],
            device_id={"rad": my_rad - 1},
        )

    def halo_up():
        return pltpu.make_async_remote_copy(
            src_ref=ind.at[:, 3], dst_ref=low, send_sem=halo_send.at[0], recv_sem=halo_recv.at[0],
            device_id={"rad": my_rad + 1},
        )

    wait_spectra(0)
    for m in range(8):
        sums = over_mixed(0, m)
        for r in range(2):
            store(sums, r * 16, 192 + r * 8, 64, m)
            store(sums, r * 16 + 8, 192 + 128 + r * 8, 48, m)
    keep_induction(0)

    @pl.when(below)
    def _():
        halo_down().start()

    wait_modes(2)
    trail = jnp.where((lane >> 5) == 1, later(1), trail)
    send_spectra(2)

    pltpu.make_async_copy(erecv, erecv, e_recv.at[0]).wait()
    ered[...] = jnp.sum(erecv[...], axis=0, keepdims=True)
    mine = lax.rem(me, 16)

    def send_row(i, carry):
        pltpu.make_async_remote_copy(
            src_ref=ered.at[0],
            dst_ref=efin.at[mine],
            send_sem=e_send.at[1],
            recv_sem=e_recv.at[1],
            device_id={"harm": me - mine + lax.rem(mine + i, 16)},
        ).start()
        return carry

    lax.fori_loop(1, 16, send_row, 0)
    pltpu.make_async_copy(ered.at[0], efin.at[mine], e_recv.at[1]).start()

    wait_modes(3)
    trail = jnp.where((lane >> 5) == 2, later(2), trail)
    send_spectra(3)
    spec[4] = trail.astype(BF16)
    send_spectra(4)

    wait_spectra(1)
    wait_spectra(2)
    for m in range(8):
        acc[m] = over_rows([column(1, m), column(2, m)], m, (0, 1))
    wait_spectra(3)
    for m in range(8):
        sums = acc[m] + over_rows([column(3, m)], m, (2,))
        for r in range(2):
            store(sums, r * 32, 192 + 48 + r * 8, 64, m)
            for c in range(3):
                store(sums, r * 32 + 8 + c * 8, 192 + c * 64 + 16 + r * 8, 16, m)
                store(sums, 64 + r * 32 + c * 8, c * 64 + r * 8, 48, m)
            store(sums, 64 + r * 32 + 24, 16 + r * 8, 16, m)
    keep_induction(3)

    @pl.when(above)
    def _():
        halo_down().wait_recv()
        halo_up().start()

    keep_induction(1)
    keep_induction(2)

    wait_spectra(4)
    for m in range(8):
        sums = over_mixed(4, m)
        for r in range(2):
            for c in (1, 2):
                store(sums, r * 16 + (c - 1) * 8, c * 64 + 16 + r * 8, 16, m)

    for half in range(2):
        lanes = pl.ds(half * 128, 128)
        adv[:, :, :, :, lanes] = out[half, 0:192, :].reshape(3, 4, 2, 8, 128).astype(BF16)
    pltpu.make_async_copy(efin, efin, e_recv.at[1]).wait()
    for q in range(2):
        for s in range(4):
            for half in range(2):
                energy[q, s:s + 1, half * 128:(half + 1) * 128] = efin[(q * 4 + s) * 2 + half]

    shells = [ind[:, s].astype(F32) for s in range(4)]
    grad[:, 1] = ((shells[2] - shells[0]) * 0.5).astype(BF16)
    grad[:, 2] = ((shells[3] - shells[1]) * 0.5).astype(BF16)

    @pl.when(below)
    def _():
        halo_down().wait_send()
        halo_up().wait_recv()

    grad[:, 0] = ((shells[1] - low[...].astype(F32)) * 0.5).astype(BF16)

    @pl.when(above)
    def _():
        halo_up().wait_send()

    grad[:, 3] = ((high[...].astype(F32) - shells[2]) * 0.5).astype(BF16)

    others = pl.ds(0, (HARM - 1) * 8)
    for group in range(4):
        sent = mode_part(wire, group, others)
        pltpu.make_async_copy(sent, sent, mode_send.at[group]).wait()
    for group in range(5):
        sent = spec.at[group, others, :]
        pltpu.make_async_copy(sent, sent, spec_send.at[group]).wait()
    pltpu.make_async_copy(erecv.at[pl.ds(0, 31)], erecv.at[pl.ds(0, 31)], e_send.at[0]).wait()
    pltpu.make_async_copy(efin.at[pl.ds(0, 15)], efin.at[pl.ds(0, 15)], e_send.at[1]).wait()


def hand_out(adv, grad, energy, adv_out, grad_out, energy_out, sem):
    copies = [
        pltpu.make_async_copy(source, target, sem.at[i])
        for i, (source, target) in enumerate(
            ((adv, adv_out), (grad, grad_out), (energy, energy_out))
        )
    ]
    for copy in copies:
        copy.start()
    for copy in copies:
        copy.wait()


def local(velocity, magnetic, vorticity, current):
    vmem = pl.BlockSpec(memory_space=pltpu.VMEM)
    block = velocity.shape
    made = pl.pallas_call(
        kernel,
        out_shape=(
            jax.ShapeDtypeStruct(block, BF16),
            jax.ShapeDtypeStruct(block, BF16),
            jax.ShapeDtypeStruct((2, 4, L), F32),
        ),
        in_specs=[pl.BlockSpec(memory_space=pltpu.HBM)] * 4,
        out_specs=(vmem,) * 3,
        scratch_shapes=[
            pltpu.VMEM((4,) + block, BF16),
            pltpu.VMEM((2, L * 8, 128), F32),
            pltpu.VMEM((8, 192, L), BF16),
            pltpu.VMEM((2, 48 * 64, 128), F32),
            pltpu.VMEM((8, 384, 512), BF16),
            pltpu.VMEM((3, 3, 256, 128), F32),
            pltpu.VMEM((3, 3, 256, 128), BF16),
            pltpu.VMEM((3, 3, 256, 128), BF16),
            pltpu.VMEM((2, 256, NPHI), BF16),
            pltpu.VMEM((256, 256), BF16),
            pltpu.VMEM((3, 128, 256), BF16),
            pltpu.VMEM((128, NPHI), F32),
            pltpu.VMEM((192, NPHI), F32),
            pltpu.VMEM((3, 256, NPHI), BF16),
            pltpu.VMEM((128, NPHI), BF16),
            pltpu.VMEM((5, 256, 128), BF16),
            pltpu.VMEM((5, 256, 128), BF16),
            pltpu.VMEM((5, 256, 128), F32),
            pltpu.VMEM((8, 128, L), F32),
            pltpu.VMEM((2, 384, 128), F32),
            pltpu.VMEM((3, 4, 2, 8, L), BF16),
            pltpu.VMEM((3, 2, 8, L), BF16),
            pltpu.VMEM((3, 2, 8, L), BF16),
            pltpu.VMEM((16, 1, 128), F32),
            pltpu.VMEM((HARM, 1, 128), F32),
            pltpu.VMEM((1, 1, 128), F32),
            pltpu.VMEM((16, 1, 128), F32),
            pltpu.SemaphoreType.DMA((4,)),
            pltpu.SemaphoreType.DMA((4,)),
            pltpu.SemaphoreType.DMA((4,)),
            pltpu.SemaphoreType.DMA((5,)),
            pltpu.SemaphoreType.DMA((5,)),
            pltpu.SemaphoreType.DMA((2,)),
            pltpu.SemaphoreType.DMA((2,)),
            pltpu.SemaphoreType.DMA((2,)),
            pltpu.SemaphoreType.DMA((2,)),
        ],
        compiler_params=pltpu.CompilerParams(
            collective_id=0, has_side_effects=True, vmem_limit_bytes=40 * 1024 * 1024
        ),
    )(*(pltpu.with_memory_space_constraint(v, pltpu.HBM) for v in (velocity, magnetic, vorticity, current)))
    return pl.pallas_call(
        hand_out,
        out_shape=tuple(jax.ShapeDtypeStruct(v.shape, v.dtype) for v in made),
        in_specs=[pl.BlockSpec(memory_space=pl.ANY)] * 3,
        out_specs=(pl.BlockSpec(memory_space=pltpu.HBM),) * 3,
        scratch_shapes=[pltpu.SemaphoreType.DMA((3,))],
        compiler_params=pltpu.CompilerParams(vmem_limit_bytes=1024 * 1024),
    )(*made)


def solution(mesh):
    split = P(None, "rad", None, "harm", None)
    return jax.shard_map(
        local,
        mesh=mesh,
        in_specs=(split,) * 4,
        out_specs=(split, split, P(None, "rad", None)),
        check_vma=False,
    )
```
